256 devices in a mesh: seq: 16 (over z, core), tp: 16 (over y, x).
Axes of the slice: x: 4, y: 4, z: 8, core: 2. Of those that a mesh axis runs over, the one named last changes fastest.
Arguments:
- latents: bfloat16 [16, 8192, 512], P(None, ('seq', 'tp')), may hold values from -6 to 6
- rotary_rows: bfloat16 [16, 8192, 64], P(None, ('seq', 'tp')), may hold values from -6 to 6
- latent_gain: float32 [512], replicated, may hold values from 0.25 to 1.75
- key_up: bfloat16 [512, 16, 128], P(None, 'tp'), may hold values from -0.25 to 0.25
- value_up: bfloat16 [512, 16, 128], P(None, 'tp'), may hold values from -0.25 to 0.25
Outputs:
- decode_keys: bfloat16 [16, 16, 192, 8192], P('seq', 'tp')
- decode_values: bfloat16 [16, 8192, 16, 128], P('seq', None, 'tp')
The draws below stay inside these ranges and needn't reach their ends.
All inputs are finite; a program needn't handle non-finite values.
Results may differ from the reference program's by a relative error of at most 0.0049.
Values may be sent and summed in bfloat16 or wider, within the bound.
A program may use at most 64 MiB of HBM per device.

```python
import jax
import jax.numpy as jnp
from jax import lax

BATCH = 16
LENGTH = 8192
HEADS = 16
LATENT = 512
KEY_PART = 128
ROTARY = 64
VALUE_SIZE = 128


def levels(own_key, dims, shards, smallest, high):
    def one(dim, blocks):
        steps = jax.random.uniform(jax.random.fold_in(jax.random.fold_in(own_key, 6), dim), (blocks,), jnp.float32, smallest / len(shards), high / len(shards))
        return jnp.repeat(jnp.exp(steps), dims[dim] // blocks).reshape((-1,) + (1,) * (len(dims) - dim - 1))

    loudness = one(*shards[0])
    for cut in shards[1:]:
        loudness = loudness * one(*cut)
    return loudness


def bell_draw(rng, dims, width, limit, split=(), held_as=jnp.bfloat16):
    factor_of = levels(rng, dims, split, -0.22, 0.18) if split else 1.0
    array = jax.random.normal(rng, dims, jnp.float32) * width * factor_of
    return jnp.minimum(jnp.maximum(array, -limit), limit).astype(held_as)


def setup_inputs(seed: int = 0) -> dict:
    arg_keys = jax.random.split(jax.random.key(seed), 6)
    latents = bell_draw(arg_keys[0], (BATCH, LENGTH, LATENT), 1.0, 6.0, ((1, 256),))
    rotary_rows = bell_draw(arg_keys[1], (BATCH, LENGTH, ROTARY), 1.0, 6.0, ((1, 256),))
    latent_gain = jnp.clip(1.0 + 0.15 * jax.random.normal(arg_keys[2], (LATENT,), jnp.float32), 0.25, 1.75)
    key_up = bell_draw(arg_keys[3], (LATENT, HEADS, KEY_PART), LATENT ** -0.5, 0.25, ((1, 16),))
    value_up = bell_draw(arg_keys[4], (LATENT, HEADS, VALUE_SIZE), LATENT ** -0.5, 0.25, ((1, 16),))
    return dict(latents=latents, rotary_rows=rotary_rows, latent_gain=latent_gain, key_up=key_up, value_up=value_up)


def root_norm(vectors, row_gain):
    return vectors * lax.rsqrt(lax.optimization_barrier(jnp.mean(vectors * vectors, axis=-1, keepdims=True)) + 1e-06) * row_gain

def reference(latents, rotary_rows, latent_gain, key_up, value_up):
    rows_ready = root_norm(latents.astype(jnp.float32), latent_gain).astype(jnp.bfloat16)
    rows_ready = lax.optimization_barrier(rows_ready)

    def expand_one(one):
        rows_one, rotary_one = one
        wide_keys = jnp.einsum('tr,rhk->thk', rows_one.astype(jnp.float32), key_up.astype(jnp.float32)).astype(jnp.bfloat16)
        shared = jnp.broadcast_to(rotary_one[:, None], (LENGTH, HEADS, ROTARY))
        wide_values = jnp.einsum('tr,rhk->thk', rows_one.astype(jnp.float32), value_up.astype(jnp.float32)).astype(jnp.bfloat16)
        return (jnp.concatenate([wide_keys, shared], axis=-1), wide_values)
    decode_keys, decode_values = lax.map(expand_one, (rows_ready, rotary_rows))
    decode_keys = jnp.transpose(decode_keys, (0, 2, 3, 1))
    return (decode_keys, decode_values)
```

```python
import functools

import jax
import jax.numpy as jnp
from jax import lax
from jax.experimental import pallas as pl
from jax.experimental.pallas import tpu as pltpu
from jax.sharding import PartitionSpec as P

SEQ, TP, RING = 16, 16, 4
ROWS, WIDTH, ROT, HEAD = 32, 512, 64, 128
PACKED = ROWS * WIDTH // 128 + ROWS * ROT // 128
CHUNKS = WIDTH // 128
FLAT = CHUNKS * ROWS
UNIT = TP * ROWS
D1, D2, D3, D4 = 1, 2, 3, 5


def kernel(
    lat_ref, rot_ref, gain_ref, wk_ref, wv_ref, keys_ref, values_ref,
    own, held, weights, spread, send_sem, recv_sem,
):
    seq, tp = lax.axis_index("seq"), lax.axis_index("tp")
    z, core = seq // 2, seq % 2
    y, x = tp // RING, tp % RING

    def seq_of(n):
        k = n // 2
        dz = ((k + 1) // 2) * (1 - 2 * ((k + 1) % 2))
        return ((z + dz + 8) % 8) * 2 + (core + n) % 2

    def tp_of(n, p, q):
        first_y = n % 2
        dy = first_y * p + (1 - first_y) * q
        dx = first_y * q + (1 - first_y) * p
        return ((y + dy + RING) % RING) * RING + (x + dx + RING) % RING

    barrier = pltpu.get_barrier_semaphore()

    def greet(n, _):
        pl.semaphore_signal(barrier, inc=1, device_id=(seq_of(n), tp))
        return _

    lax.fori_loop(1, SEQ, greet, 0)
    for p, q in ((1, 0), (-1, 0), (0, 1), (0, -1)):
        pl.semaphore_signal(barrier, inc=1, device_id=(seq, tp_of(0, p, q)))

    def prepare(s, _):
        rows = lat_ref[s].astype(jnp.float32)
        scale = lax.rsqrt(jnp.mean(rows * rows, axis=-1, keepdims=True) + 1e-06)
        ready = (rows * scale * gain_ref[...]).astype(jnp.bfloat16)
        for c in range(CHUNKS):
            own[s, c * ROWS : (c + 1) * ROWS, :] = ready[:, c * 128 : (c + 1) * 128]
        rot = rot_ref[s]
        own[s, FLAT:PACKED, :] = jnp.concatenate(
            [rot[: ROWS // 2], rot[ROWS // 2 :]], axis=-1
        )
        return _

    lax.fori_loop(0, SEQ, prepare, 0)
    held[seq * TP + tp] = own[seq]
    weights[:, :HEAD] = wk_ref[...]
    weights[:, HEAD:] = wv_ref[...]
    row = lax.broadcasted_iota(jnp.int32, (64, 128), 0)
    lane = lax.broadcasted_iota(jnp.int32, (64, 128), 1)
    for h in range(2):
        at = (row // 16) * 32 + h * 16 + row % 16
        spread[h] = (at == lane).astype(jnp.float32).astype(jnp.bfloat16)

    pl.semaphore_wait(barrier, SEQ - 1 + 4)

    def scatter(n, _):
        pltpu.make_async_remote_copy(
            src_ref=own.at[seq_of(n)],
            dst_ref=held.at[seq * TP + tp],
            send_sem=send_sem,
            recv_sem=recv_sem.at[seq * TP + tp],
            device_id=(seq_of(n), tp),
        ).start()
        return _

    lax.fori_loop(1, SEQ, scatter, 0)

    def copy_of(slot, target):
        return pltpu.make_async_remote_copy(
            src_ref=held.at[slot],
            dst_ref=held.at[slot],
            send_sem=send_sem,
            recv_sem=recv_sem.at[slot],
            device_id=(seq, target),
        )

    def slot_of(n, p, q):
        return seq_of(n) * TP + tp_of(n, p, q)

    def arrive(n, p, q):
        copy_of(slot_of(n, p, q), tp_of(n, 1, 0)).wait_recv()

    def send(n, p, q, dp, dq):
        copy_of(slot_of(n, p, q), tp_of(n, dp, dq)).start()

    def when(n, low=0):
        return pl.when((n >= low) & (n < SEQ))

    def step(it, carry):
        n0, n1, n2, n3, n4 = it, it - D1, it - D2, it - D3, it - D4

        @when(n0, 1)
        def _():
            arrive(n0, 0, 0)

        @when(n0)
        def _():
            send(n0, 0, 0, 1, 0)
            send(n0, 0, 0, -1, 0)
            send(n0, 0, 0, 0, 1)
            send(n0, 0, 0, 0, -1)

        @when(n1)
        def _():
            way = 1 - 2 * ((n1 // 2) % 2)
            arrive(n1, 0 - way, 0)
            send(n1, 0 - way, 0, way, 0)
            send(n1, 0 - way, 0, 0, 1)
            send(n1, 0 - way, 0, 0, -1)
            arrive(n1, way, 0)
            send(n1, way, 0, 0, 1)
            send(n1, way, 0, 0, -1)

        @when(n2)
        def _():
            arrive(n2, 2, 0)
            send(n2, 2, 0, 0, 1)
            send(n2, 2, 0, 0, -1)

        @when(n3)
        def _():
            arrive(n3, 0, -1)
            send(n3, 0, -1, 0, 1)
            arrive(n3, -1, 1)
            send(n3, -1, 1, 0, -1)
            arrive(n3, 1, -1)
            send(n3, 1, -1, 0, 1)
            arrive(n3, 2, 1)
            send(n3, 2, 1, 0, -1)

        @when(n4)
        def _():
            arrive(n4, 0, 1)
            arrive(n4, 1, 1)
            arrive(n4, -1, -1)
            arrive(n4, 2, -1)
            for p in (0, -1, 1, 2):
                arrive(n4, p, 2)
            u = seq_of(n4)
            for q in range(TP // 4):
                block = held[pl.ds(u * TP + 4 * q, 4)]
                rows = jnp.concatenate(
                    [
                        block[:, c * ROWS : (c + 1) * ROWS, :].reshape(4 * ROWS, 128)
                        for c in range(CHUNKS)
                    ],
                    axis=-1,
                )
                wide = jnp.dot(rows, weights[...], preferred_element_type=jnp.float32)
                at = pl.multiple_of(u * UNIT + q * 128, 128)
                values_ref[pl.ds(at, 128), :] = wide[:, HEAD:].astype(jnp.bfloat16)
                keys_ref[:HEAD, pl.ds(at, 128)] = wide[:, :HEAD].T.astype(jnp.bfloat16)
                rot = block[:, FLAT:, :].reshape(64, 128).astype(jnp.float32).T
                rot = rot.astype(jnp.bfloat16)
                turned = jnp.dot(
                    rot[:ROT], spread[0], preferred_element_type=jnp.float32
                ) + jnp.dot(rot[ROT:], spread[1], preferred_element_type=jnp.float32)
                keys_ref[HEAD:, pl.ds(at, 128)] = turned.astype(jnp.bfloat16)

        return carry

    lax.fori_loop(0, SEQ + D4, step, 0)
    sent = SEQ * TP - 1
    pltpu.make_async_copy(held.at[pl.ds(0, sent)], held.at[pl.ds(0, sent)], send_sem).wait()


def shards(latents, rotary_rows, latent_gain, key_up, value_up):
    length = SEQ * UNIT
    vmem = pl.BlockSpec(memory_space=pltpu.VMEM)
    keys, values = pl.pallas_call(
        kernel,
        out_shape=(
            jax.ShapeDtypeStruct((HEAD + ROT, length), jnp.bfloat16),
            jax.ShapeDtypeStruct((length, HEAD), jnp.bfloat16),
        ),
        in_specs=[vmem] * 5,
        out_specs=(vmem, vmem),
        scratch_shapes=[
            pltpu.VMEM((SEQ, PACKED, 128), jnp.bfloat16),
            pltpu.VMEM((SEQ * TP, PACKED, 128), jnp.bfloat16),
            pltpu.VMEM((WIDTH, 2 * HEAD), jnp.bfloat16),
            pltpu.VMEM((2, 64, 128), jnp.bfloat16),
            pltpu.SemaphoreType.DMA,
            pltpu.SemaphoreType.DMA((SEQ * TP,)),
        ],
        compiler_params=pltpu.CompilerParams(collective_id=0, has_side_effects=True),
        name="gather_and_expand",
    )(
        latents,
        rotary_rows,
        latent_gain.reshape(1, WIDTH),
        key_up.reshape(WIDTH, HEAD),
        value_up.reshape(WIDTH, HEAD),
    )
    return keys[None, None], values[None, :, None]


def solution(mesh):
    return jax.shard_map(
        shards,
        mesh=mesh,
        in_specs=(
            P(None, ("seq", "tp"), None),
            P(None, ("seq", "tp"), None),
            P(),
            P(None, "tp", None),
            P(None, "tp", None),
        ),
        out_specs=(P("seq", "tp", None, None), P("seq", None, "tp", None)),
        check_vma=False,
    )
```

```python
import functools

import jax
import jax.numpy as jnp
from jax import lax
from jax.experimental import pallas as pl
from jax.experimental.pallas import tpu as pltpu
from jax.sharding import PartitionSpec as P

SEQ, TP, RING = 16, 16, 4
ROWS, WIDTH, ROT, HEAD = 32, 512, 64, 128
PACKED = ROWS * WIDTH // 128 + ROWS * ROT // 128
CHUNKS = WIDTH // 128
FLAT = CHUNKS * ROWS
UNIT = TP * ROWS
D1, D2, D3, D4 = 2, 4, 9, 14


def kernel(
    lat_hbm, rot_hbm, gain_hbm, wk_hbm, wv_hbm, keys_ref, values_ref,
    lat_ref, rot_ref, gain_ref, wk_ref, wv_ref,
    own, held, weights, spread, load_sem, send_sem, recv_sem,
):
    seq, tp = lax.axis_index("seq"), lax.axis_index("tp")
    z, core = seq // 2, seq % 2
    y, x = tp // RING, tp % RING

    def seq_of(n):
        k = n // 2
        dz = ((k + 1) // 2) * (1 - 2 * ((k + 1) % 2))
        return ((z + dz + 8) % 8) * 2 + (core + n) % 2

    def tp_of(n, p, q):
        first_y = n % 2
        dy = first_y * p + (1 - first_y) * q
        dx = first_y * q + (1 - first_y) * p
        return ((y + dy + RING) % RING) * RING + (x + dx + RING) % RING

    loads = [
        pltpu.make_async_copy(source, target, load_sem.at[i])
        for i, (source, target) in enumerate(
            (
                (lat_hbm, lat_ref),
                (gain_hbm, gain_ref),
                (rot_hbm, rot_ref),
                (wk_hbm, wk_ref),
                (wv_hbm, wv_ref),
            )
        )
    ]
    for load in loads:
        load.start()
    barrier = pltpu.get_barrier_semaphore()

    def greet(n, _):
        pl.semaphore_signal(barrier, inc=1, device_id=(seq_of(n), tp))
        return _

    lax.fori_loop(1, SEQ, greet, 0)
    for p, q in ((1, 0), (-1, 0), (0, 1), (0, -1)):
        pl.semaphore_signal(barrier, inc=1, device_id=(seq, tp_of(0, p, q)))

    for load in loads[:3]:
        load.wait()

    def prepare(s, _):
        rows = lat_ref[s].astype(jnp.float32)
        scale = lax.rsqrt(jnp.mean(rows * rows, axis=-1, keepdims=True) + 1e-06)
        ready = (rows * scale * gain_ref[...]).astype(jnp.bfloat16)
        for c in range(CHUNKS):
            own[s, c * ROWS : (c + 1) * ROWS, :] = ready[:, c * 128 : (c + 1) * 128]
        rot = rot_ref[s]
        own[s, FLAT:PACKED, :] = jnp.concatenate(
            [rot[: ROWS // 2], rot[ROWS // 2 :]], axis=-1
        )
        return _

    lax.fori_loop(0, SEQ, prepare, 0)
    held[seq * TP + tp] = own[seq]
    for load in loads[3:]:
        load.wait()
    weights[:, :HEAD] = wk_ref[...]
    weights[:, HEAD:] = wv_ref[...]
    row = lax.broadcasted_iota(jnp.int32, (64, 128), 0)
    lane = lax.broadcasted_iota(jnp.int32, (64, 128), 1)
    for h in range(2):
        at = (row // 16) * 32 + h * 16 + row % 16
        spread[h] = (at == lane).astype(jnp.float32).astype(jnp.bfloat16)

    pl.semaphore_wait(barrier, SEQ - 1 + 4)

    def scatter(n, _):
        pltpu.make_async_remote_copy(
            src_ref=own.at[seq_of(n)],
            dst_ref=held.at[seq * TP + tp],
            send_sem=send_sem,
            recv_sem=recv_sem.at[seq * TP + tp],
            device_id=(seq_of(n), tp),
        ).start()
        return _

    lax.fori_loop(1, SEQ, scatter, 0)

    def copy_of(slot, target):
        return pltpu.make_async_remote_copy(
            src_ref=held.at[slot],
            dst_ref=held.at[slot],
            send_sem=send_sem,
            recv_sem=recv_sem.at[slot],
            device_id=(seq, target),
        )

    def slot_of(n, p, q):
        return seq_of(n) * TP + tp_of(n, p, q)

    def arrive(n, p, q):
        copy_of(slot_of(n, p, q), tp_of(n, 1, 0)).wait_recv()

    def send(n, p, q, dp, dq):
        copy_of(slot_of(n, p, q), tp_of(n, dp, dq)).start()

    def when(n, low=0):
        return pl.when((n >= low) & (n < SEQ))

    def step(it, carry):
        n0, n1, n2, n3, n4 = it, it - D1, it - D2, it - D3, it - D4

        @when(n0, 1)
        def _():
            arrive(n0, 0, 0)

        @when(n0)
        def _():
            send(n0, 0, 0, 1, 0)
            send(n0, 0, 0, -1, 0)
            send(n0, 0, 0, 0, 1)
            send(n0, 0, 0, 0, -1)

        @when(n1)
        def _():
            way = 1 - 2 * ((n1 // 2) % 2)
            arrive(n1, 0 - way, 0)
            send(n1, 0 - way, 0, way, 0)
            send(n1, 0 - way, 0, 0, 1)
            send(n1, 0 - way, 0, 0, -1)
            arrive(n1, way, 0)
            send(n1, way, 0, 0, 1)
            send(n1, way, 0, 0, -1)

        @when(n2)
        def _():
            arrive(n2, 2, 0)
            send(n2, 2, 0, 0, 1)
            send(n2, 2, 0, 0, -1)

        @when(n3)
        def _():
            arrive(n3, 0, -1)
            send(n3, 0, -1, 0, 1)
            arrive(n3, -1, 1)
            send(n3, -1, 1, 0, -1)
            arrive(n3, 1, -1)
            send(n3, 1, -1, 0, 1)
            arrive(n3, 2, 1)
            send(n3, 2, 1, 0, -1)

        @when(n4)
        def _():
            arrive(n4, 0, 1)
            arrive(n4, 1, 1)
            arrive(n4, -1, -1)
            arrive(n4, 2, -1)
            for p in (0, -1, 1, 2):
                arrive(n4, p, 2)
            u = seq_of(n4)
            for q in range(TP // 4):
                block = held[pl.ds(u * TP + 4 * q, 4)]
                rows = jnp.concatenate(
                    [
                        block[:, c * ROWS : (c + 1) * ROWS, :].reshape(4 * ROWS, 128)
                        for c in range(CHUNKS)
                    ],
                    axis=-1,
                )
                wide = jnp.dot(rows, weights[...], preferred_element_type=jnp.float32)
                at = pl.multiple_of(u * UNIT + q * 128, 128)
                values_ref[pl.ds(at, 128), :] = wide[:, HEAD:].astype(jnp.bfloat16)
                keys_ref[:HEAD, pl.ds(at, 128)] = wide[:, :HEAD].T.astype(jnp.bfloat16)
                rot = block[:, FLAT:, :].reshape(64, 128).astype(jnp.float32).T
                rot = rot.astype(jnp.bfloat16)
                turned = jnp.dot(
                    rot[:ROT], spread[0], preferred_element_type=jnp.float32
                ) + jnp.dot(rot[ROT:], spread[1], preferred_element_type=jnp.float32)
                keys_ref[HEAD:, pl.ds(at, 128)] = turned.astype(jnp.bfloat16)

        return carry

    lax.fori_loop(0, SEQ + D4, step, 0)
    sent = SEQ * TP - 1
    pltpu.make_async_copy(held.at[pl.ds(0, sent)], held.at[pl.ds(0, sent)], send_sem).wait()


def shards(latents, rotary_rows, latent_gain, key_up, value_up):
    length = SEQ * UNIT
    vmem = pl.BlockSpec(memory_space=pltpu.VMEM)
    keys, values = pl.pallas_call(
        kernel,
        out_shape=(
            pltpu.VMEM((HEAD + ROT, length), jnp.bfloat16),
            pltpu.VMEM((length, HEAD), jnp.bfloat16),
        ),
        in_specs=[pl.BlockSpec(memory_space=pltpu.HBM)] * 5,
        out_specs=(vmem, vmem),
        scratch_shapes=[
            pltpu.VMEM((SEQ, ROWS, WIDTH), jnp.bfloat16),
            pltpu.VMEM((SEQ, ROWS, ROT), jnp.bfloat16),
            pltpu.VMEM((1, WIDTH), jnp.float32),
            pltpu.VMEM((WIDTH, HEAD), jnp.bfloat16),
            pltpu.VMEM((WIDTH, HEAD), jnp.bfloat16),
            pltpu.VMEM((SEQ, PACKED, 128), jnp.bfloat16),
            pltpu.VMEM((SEQ * TP, PACKED, 128), jnp.bfloat16),
            pltpu.VMEM((WIDTH, 2 * HEAD), jnp.bfloat16),
            pltpu.VMEM((2, 64, 128), jnp.bfloat16),
            pltpu.SemaphoreType.DMA((5,)),
            pltpu.SemaphoreType.DMA,
            pltpu.SemaphoreType.DMA((SEQ * TP,)),
        ],
        compiler_params=pltpu.CompilerParams(collective_id=0, has_side_effects=True, vmem_limit_bytes=24 * 2**20),
        name="gather_and_expand",
    )(
        *(
            pltpu.with_memory_space_constraint(a, pltpu.HBM)
            for a in (
                latents,
                rotary_rows,
                latent_gain.reshape(1, WIDTH),
                key_up.reshape(WIDTH, HEAD),
                value_up.reshape(WIDTH, HEAD),
            )
        )
    )
    return keys[None, None], values[None, :, None]


def solution(mesh):
    return jax.shard_map(
        shards,
        mesh=mesh,
        in_specs=(
            P(None, ("seq", "tp"), None),
            P(None, ("seq", "tp"), None),
            P(),
            P(None, "tp", None),
            P(None, "tp", None),
        ),
        out_specs=(P("seq", "tp", None, None), P("seq", None, "tp", None)),
        check_vma=False,
    )
```

```python
import functools

import jax
import jax.numpy as jnp
from jax import lax
from jax.experimental import pallas as pl
from jax.experimental.pallas import tpu as pltpu
from jax.sharding import PartitionSpec as P

SEQ, TP, RING = 16, 16, 4
ROWS, WIDTH, ROT, HEAD = 32, 512, 64, 128
PACKED = ROWS * WIDTH // 128 + ROWS * ROT // 128
CHUNKS = WIDTH // 128
FLAT = CHUNKS * ROWS
LINE = RING * ROWS
WIDE = 2 * LINE + RING * (PACKED - FLAT)
UNIT = TP * ROWS
D1, D2, D3, D4 = 5, 9, 13, 19
RELAY = 3


def kernel(
    lat_hbm, rot_hbm, gain_hbm, wk_hbm, wv_hbm, keys_ref, values_ref,
    lat_ref, rot_ref, gain_ref, own, held, weights, spread,
    key_rows, rot_rows, wide_out, wide_in,
    load_sem, send_sem, recv_sem, wide_send, wide_recv, up_send, up_recv,
):
    seq, tp = lax.axis_index("seq"), lax.axis_index("tp")
    z, core = seq // 2, seq % 2
    y, x = tp // RING, tp % RING

    def seq_of(n):
        k = n // 2
        dz = ((k + 1) // 2) * (1 - 2 * ((k + 1) % 2))
        return ((z + dz + 8) % 8) * 2 + (core + n) % 2

    def tp_of(n, p, q):
        first_y = n % 2
        dy = first_y * p + (1 - first_y) * q
        dx = first_y * q + (1 - first_y) * p
        return ((y + dy + RING) % RING) * RING + (x + dx + RING) % RING

    def line_of(n, q, j):
        first_y = n % 2
        at = (first_y * x + (1 - first_y) * y + q + RING) % RING
        return at * (RING - (RING - 1) * first_y) + j * (1 + (RING - 1) * first_y)

    def up_of(n, q):
        return 1 + 2 * (1 - n % 2) + (1 - q) // 2

    def way_of(n):
        return 1 - 2 * ((n // 4) % 2)

    def side_of(n):
        return 1 - 2 * ((n // 2) % 2)

    loads = [
        pltpu.make_async_copy(source, target, load_sem.at[i])
        for i, (source, target) in enumerate(
            (
                (lat_hbm, lat_ref),
                (gain_hbm, gain_ref),
                (rot_hbm, rot_ref),
                (wk_hbm, weights.at[0, 0]),
                (wv_hbm, weights.at[0, 1]),
            )
        )
    ]
    for load in loads:
        load.start()
    barrier = pltpu.get_barrier_semaphore()

    def greet(n, _):
        pl.semaphore_signal(barrier, inc=1, device_id=(seq_of(n), tp))
        return _

    lax.fori_loop(1, SEQ, greet, 0)
    around = [tp_of(0, 1, 0), tp_of(0, -1, 0), tp_of(0, 0, 1), tp_of(0, 0, -1)]
    for target in around:
        pl.semaphore_signal(barrier, inc=1, device_id=(seq, target))

    for load in loads[:3]:
        load.wait()

    def prepare(s, _):
        rows = lat_ref[s].astype(jnp.float32)
        scale = lax.rsqrt(jnp.mean(rows * rows, axis=-1, keepdims=True) + 1e-06)
        ready = (rows * scale * gain_ref[...]).astype(jnp.bfloat16)
        for c in range(CHUNKS):
            own[s, c * ROWS : (c + 1) * ROWS, :] = ready[:, c * 128 : (c + 1) * 128]
        rot = rot_ref[s]
        own[s, FLAT:PACKED, :] = jnp.concatenate(
            [rot[: ROWS // 2], rot[ROWS // 2 :]], axis=-1
        )
        return _

    lax.fori_loop(0, SEQ, prepare, 0)
    held[seq * TP + tp] = own[seq]
    for load in loads[3:]:
        load.wait()
    row = lax.broadcasted_iota(jnp.int32, (64, 128), 0)
    lane = lax.broadcasted_iota(jnp.int32, (64, 128), 1)
    for h in range(2):
        at = (row // 16) * 32 + h * 16 + row % 16
        spread[h] = (at == lane).astype(jnp.float32).astype(jnp.bfloat16)

    pl.semaphore_wait(barrier, SEQ - 1 + 4)

    def scatter(n, _):
        pltpu.make_async_remote_copy(
            src_ref=own.at[seq_of(n)],
            dst_ref=held.at[seq * TP + tp],
            send_sem=send_sem,
            recv_sem=recv_sem.at[seq * TP + tp],
            device_id=(seq_of(n), tp),
        ).start()
        return _

    lax.fori_loop(1, SEQ, scatter, 0)

    def share(source, target, half, device):
        return pltpu.make_async_remote_copy(
            src_ref=weights.at[source, half],
            dst_ref=weights.at[target, half],
            send_sem=up_send,
            recv_sem=up_recv.at[target, half],
            device_id=device,
        )

    partner = (z * 2 + 1 - core, tp)
    for k, target in enumerate(around):
        back = 1 + k + 1 - 2 * (k % 2)
        share(0, back, core, (seq, target)).start()

    def copy_of(slot, target):
        return pltpu.make_async_remote_copy(
            src_ref=held.at[slot],
            dst_ref=held.at[slot],
            send_sem=send_sem,
            recv_sem=recv_sem.at[slot],
            device_id=(seq, target),
        )

    def slot_of(n, p, q):
        return seq_of(n) * TP + tp_of(n, p, q)

    def arrive(n, p, q):
        copy_of(slot_of(n, p, q), tp_of(n, 1, 0)).wait_recv()

    def send(n, p, q, dp, dq):
        copy_of(slot_of(n, p, q), tp_of(n, dp, dq)).start()

    def wide_copy(n, which, q):
        return pltpu.make_async_remote_copy(
            src_ref=wide_out.at[n, which],
            dst_ref=wide_in.at[n, which],
            send_sem=wide_send,
            recv_sem=wide_recv.at[n, which],
            device_id=(seq, tp_of(n, 0, q)),
        )

    def times(rows, k):
        both = jnp.concatenate([weights[k, 0], weights[k, 1]], axis=-1)
        wide = jnp.dot(rows, both, preferred_element_type=jnp.float32)
        return wide.astype(jnp.bfloat16)

    def place(n, device, keys, values, rot):
        key_rows[n, pl.ds(pl.multiple_of(device * ROWS, ROWS), ROWS), :] = keys
        at = pl.multiple_of(seq_of(n) * UNIT + device * ROWS, ROWS)
        values_ref[pl.ds(at, ROWS), :] = values
        rot_rows[n, pl.ds(pl.multiple_of(device * 16, 16), 16), :] = rot

    def expand(n, q, which, target):
        blocks = [held[seq_of(n) * TP + line_of(n, q, j)] for j in range(RING)]
        rows = jnp.concatenate(
            [
                jnp.concatenate(
                    [b[c * ROWS : (c + 1) * ROWS] for c in range(CHUNKS)], axis=-1
                )
                for b in blocks
            ],
            axis=0,
        )
        other = times(rows, up_of(n, target))
        wide_out[n, which, :LINE, :] = other[:, :HEAD]
        wide_out[n, which, LINE : 2 * LINE, :] = other[:, HEAD:]
        mine = times(rows, 0)
        for j, b in enumerate(blocks):
            at = slice(j * ROWS, (j + 1) * ROWS)
            wide_out[n, which, 2 * LINE + 16 * j : 2 * LINE + 16 * (j + 1), :] = b[FLAT:]
            place(n, line_of(n, q, j), mine[at, :HEAD], mine[at, HEAD:], b[FLAT:])

    def finish(n, which, q):
        for j in range(RING):
            at = j * ROWS
            place(
                n,
                line_of(n, q, j),
                wide_in[n, which, at : at + ROWS, :],
                wide_in[n, which, LINE + at : LINE + at + ROWS, :],
                wide_in[n, which, 2 * LINE + 16 * j : 2 * LINE + 16 * (j + 1), :],
            )

    def when(n, low=0):
        return pl.when((n >= low) & (n < SEQ))

    def step(it, carry):
        n0, n1, n2, n3, n4 = it, it - D1, it - D2, it - D3, it - D4

        @when(n0, 1)
        def _():
            arrive(n0, 0, 0)

        @when(n0)
        def _():
            send(n0, 0, 0, 0, side_of(n0))
            send(n0, 0, 0, 1, 0)
            send(n0, 0, 0, -1, 0)

        @pl.when(it == RELAY)
        def _():
            for k in range(1, 5):
                share(k, k, core, partner).wait_recv()
                share(k, k, core, partner).start()

        @when(n1)
        def _():
            way, side = way_of(n1), side_of(n1)
            arrive(n1, 0 - way, 0)
            send(n1, 0 - way, 0, way, 0)
            send(n1, 0 - way, 0, 0, side)
            arrive(n1, way, 0)
            send(n1, way, 0, 0, side)

        @pl.when(it == D2)
        def _():
            for k in range(1, 5):
                share(k, k, 1 - core, partner).wait_recv()

        @when(n2)
        def _():
            side = side_of(n2)
            arrive(n2, 2, 0)
            send(n2, 2, 0, 0, side)
            expand(n2, 0, 0, 0 - side)

        @when(n3)
        def _():
            side = side_of(n3)
            for p in (0, -1, 1, 2):
                arrive(n3, p, 0 - side)
            expand(n3, 0 - side, 1, side)

        @when(n2)
        def _():
            wide_copy(n2, 0, 0 - side_of(n2)).start()

        @when(n4)
        def _():
            side = side_of(n4)
            wide_copy(n4, 0, side).wait_recv()
            wide_copy(n4, 1, side).wait_recv()
            finish(n4, 0, side)
            finish(n4, 1, 2)
            for q in range(TP // 4):
                at = pl.multiple_of(seq_of(n4) * UNIT + q * 128, 128)
                part = key_rows[n4, q * 128 : (q + 1) * 128, :].astype(jnp.float32)
                keys_ref[:HEAD, pl.ds(at, 128)] = part.T.astype(jnp.bfloat16)
                rot = rot_rows[n4, q * 64 : (q + 1) * 64, :].astype(jnp.float32).T
                rot = rot.astype(jnp.bfloat16)
                turned = jnp.dot(
                    rot[:ROT], spread[0], preferred_element_type=jnp.float32
                ) + jnp.dot(rot[ROT:], spread[1], preferred_element_type=jnp.float32)
                keys_ref[HEAD:, pl.ds(at, 128)] = turned.astype(jnp.bfloat16)

        @when(n3)
        def _():
            wide_copy(n3, 1, side_of(n3)).start()

        return carry

    lax.fori_loop(0, SEQ + D4, step, 0)
    sent = held.at[pl.ds(0, SEQ - 1 + 7 * SEQ)]
    pltpu.make_async_copy(sent, sent, send_sem).wait()
    pltpu.make_async_copy(wide_out, wide_out, wide_send).wait()
    shared = weights.at[pl.ds(0, 4)]
    pltpu.make_async_copy(shared, shared, up_send).wait()


def shards(latents, rotary_rows, latent_gain, key_up, value_up):
    length = SEQ * UNIT
    vmem = pl.BlockSpec(memory_space=pltpu.VMEM)
    keys, values = pl.pallas_call(
        kernel,
        out_shape=(
            pltpu.VMEM((HEAD + ROT, length), jnp.bfloat16),
            pltpu.VMEM((length, HEAD), jnp.bfloat16),
        ),
        in_specs=[pl.BlockSpec(memory_space=pltpu.HBM)] * 5,
        out_specs=(vmem, vmem),
        scratch_shapes=[
            pltpu.VMEM((SEQ, ROWS, WIDTH), jnp.bfloat16),
            pltpu.VMEM((SEQ, ROWS, ROT), jnp.bfloat16),
            pltpu.VMEM((1, WIDTH), jnp.float32),
            pltpu.VMEM((SEQ, PACKED, 128), jnp.bfloat16),
            pltpu.VMEM((SEQ * TP, PACKED, 128), jnp.bfloat16),
            pltpu.VMEM((5, 2, WIDTH, HEAD), jnp.bfloat16),
            pltpu.VMEM((2, 64, 128), jnp.bfloat16),
            pltpu.VMEM((SEQ, UNIT, HEAD), jnp.bfloat16),
            pltpu.VMEM((SEQ, TP * 16, 128), jnp.bfloat16),
            pltpu.VMEM((SEQ, 2, WIDE, 128), jnp.bfloat16),
            pltpu.VMEM((SEQ, 2, WIDE, 128), jnp.bfloat16),
            pltpu.SemaphoreType.DMA((5,)),
            pltpu.SemaphoreType.DMA,
            pltpu.SemaphoreType.DMA((SEQ * TP,)),
            pltpu.SemaphoreType.DMA,
            pltpu.SemaphoreType.DMA((SEQ, 2)),
            pltpu.SemaphoreType.DMA,
            pltpu.SemaphoreType.DMA((5, 2)),
        ],
        compiler_params=pltpu.CompilerParams(
            collective_id=0, has_side_effects=True, vmem_limit_bytes=40 * 2**20
        ),
        name="gather_and_expand",
    )(
        *(
            pltpu.with_memory_space_constraint(a, pltpu.HBM)
            for a in (
                latents,
                rotary_rows,
                latent_gain.reshape(1, WIDTH),
                key_up.reshape(WIDTH, HEAD),
                value_up.reshape(WIDTH, HEAD),
            )
        )
    )
    return keys[None, None], values[None, :, None]


def solution(mesh):
    return jax.shard_map(
        shards,
        mesh=mesh,
        in_specs=(
            P(None, ("seq", "tp"), None),
            P(None, ("seq", "tp"), None),
            P(),
            P(None, "tp", None),
            P(None, "tp", None),
        ),
        out_specs=(P("seq", "tp", None, None), P("seq", None, "tp", None)),
        check_vma=False,
    )
```

```python
import functools

import jax
import jax.numpy as jnp
from jax import lax
from jax.experimental import pallas as pl
from jax.experimental.pallas import tpu as pltpu
from jax.sharding import PartitionSpec as P

SEQ, TP, RING = 16, 16, 4
ROWS, WIDTH, ROT, HEAD = 32, 512, 64, 128
PACKED = ROWS * WIDTH // 128 + ROWS * ROT // 128
CHUNKS = WIDTH // 128
FLAT = CHUNKS * ROWS
LINE = RING * ROWS
WIDE = 2 * LINE + RING * (PACKED - FLAT)
UNIT = TP * ROWS
D1, D2, D3, D4 = 5, 9, 13, 19
RELAY = 3


def kernel(
    lat_hbm, rot_hbm, gain_hbm, wk_hbm, wv_hbm, keys_ref, values_ref,
    lat_ref, rot_ref, gain_ref, own, held, weights, spread,
    key_rows, rot_rows, wide_out, wide_in,
    load_sem, send_sem, recv_sem, wide_send, wide_recv, up_send, up_recv,
):
    seq, tp = lax.axis_index("seq"), lax.axis_index("tp")
    z, core = seq // 2, seq % 2
    y, x = tp // RING, tp % RING

    def seq_of(n):
        k = n // 2
        dz = ((k + 1) // 2) * (1 - 2 * ((k + 1) % 2))
        return ((z + dz + 8) % 8) * 2 + (core + n) % 2

    to_of = seq_of

    def tp_of(n, p, q):
        first_y = n % 2
        dy = first_y * p + (1 - first_y) * q
        dx = first_y * q + (1 - first_y) * p
        return ((y + dy + RING) % RING) * RING + (x + dx + RING) % RING

    def line_of(n, q, j):
        first_y = n % 2
        at = (first_y * x + (1 - first_y) * y + q + RING) % RING
        return at * (RING - (RING - 1) * first_y) + j * (1 + (RING - 1) * first_y)

    def up_of(n, q):
        return 1 + 2 * (1 - n % 2) + (1 - q) // 2

    def way_of(n):
        return 1 - 2 * ((n // 4) % 2)

    def side_of(n):
        return 1 - 2 * ((n // 2) % 2)

    loads = [
        pltpu.make_async_copy(source, target, load_sem.at[i])
        for i, (source, target) in enumerate(
            (
                (lat_hbm, lat_ref),
                (gain_hbm, gain_ref),
                (rot_hbm, rot_ref),
                (wk_hbm, weights.at[0, 0]),
                (wv_hbm, weights.at[0, 1]),
            )
        )
    ]
    for load in loads:
        load.start()
    barrier = pltpu.get_barrier_semaphore()

    def greet(n, _):
        pl.semaphore_signal(barrier, inc=1, device_id=(seq_of(n), tp))
        return _

    lax.fori_loop(1, SEQ, greet, 0)
    around = [tp_of(0, 1, 0), tp_of(0, -1, 0), tp_of(0, 0, 1), tp_of(0, 0, -1)]
    for target in around:
        pl.semaphore_signal(barrier, inc=1, device_id=(seq, target))

    for load in loads[:3]:
        load.wait()

    def ready(s):
        rows = lat_ref[s].astype(jnp.float32)
        scale = lax.rsqrt(jnp.mean(rows * rows, axis=-1, keepdims=True) + 1e-06)
        rows = (rows * scale * gain_ref[...]).astype(jnp.bfloat16)
        rot = rot_ref[s]
        rot = jnp.concatenate([rot[: ROWS // 2], rot[ROWS // 2 :]], axis=-1)
        return [rows[:, c * 128 : (c + 1) * 128] for c in range(CHUNKS)] + [rot]

    def put(ref, at, parts):
        for c, part in enumerate(parts):
            ref[at, c * ROWS : c * ROWS + part.shape[0], :] = part

    put(held, seq * TP + tp, ready(seq))
    row = lax.broadcasted_iota(jnp.int32, (64, 128), 0)
    lane = lax.broadcasted_iota(jnp.int32, (64, 128), 1)
    for h in range(2):
        at = (row // 16) * 32 + h * 16 + row % 16
        spread[h] = (at == lane).astype(jnp.float32).astype(jnp.bfloat16)
    for load in loads[3:]:
        load.wait()

    pl.semaphore_wait(barrier, SEQ - 1 + 4)

    def share(source, target, half, device):
        return pltpu.make_async_remote_copy(
            src_ref=weights.at[source, half],
            dst_ref=weights.at[target, half],
            send_sem=up_send,
            recv_sem=up_recv.at[target, half],
            device_id=device,
        )

    partner = (z * 2 + 1 - core, tp)
    for k, target in enumerate(around):
        back = 1 + k + 1 - 2 * (k % 2)
        share(0, back, core, (seq, target)).start()

    def copy_of(slot, target):
        return pltpu.make_async_remote_copy(
            src_ref=held.at[slot],
            dst_ref=held.at[slot],
            send_sem=send_sem,
            recv_sem=recv_sem.at[slot],
            device_id=(seq, target),
        )

    def slot_of(n, p, q):
        return seq_of(n) * TP + tp_of(n, p, q)

    def arrive(n, p, q):
        copy_of(slot_of(n, p, q), tp_of(n, 1, 0)).wait_recv()

    def send(n, p, q, dp, dq):
        copy_of(slot_of(n, p, q), tp_of(n, dp, dq)).start()

    def wide_copy(n, which, q):
        return pltpu.make_async_remote_copy(
            src_ref=wide_out.at[n, which],
            dst_ref=wide_in.at[n, which],
            send_sem=wide_send,
            recv_sem=wide_recv.at[n, which],
            device_id=(seq, tp_of(n, 0, q)),
        )

    def times(rows, k):
        both = jnp.concatenate([weights[k, 0], weights[k, 1]], axis=-1)
        wide = jnp.dot(rows, both, preferred_element_type=jnp.float32)
        return wide.astype(jnp.bfloat16)

    def place(n, device, keys, values, rot):
        key_rows[n, pl.ds(pl.multiple_of(device * ROWS, ROWS), ROWS), :] = keys
        at = pl.multiple_of(seq_of(n) * UNIT + device * ROWS, ROWS)
        values_ref[pl.ds(at, ROWS), :] = values
        rot_rows[n, pl.ds(pl.multiple_of(device * 16, 16), 16), :] = rot

    def expand(n, q, which, target):
        blocks = [held[seq_of(n) * TP + line_of(n, q, j)] for j in range(RING)]
        rows = jnp.concatenate(
            [
                jnp.concatenate(
                    [b[c * ROWS : (c + 1) * ROWS] for c in range(CHUNKS)], axis=-1
                )
                for b in blocks
            ],
            axis=0,
        )
        other = times(rows, up_of(n, target))
        wide_out[n, which, :LINE, :] = other[:, :HEAD]
        wide_out[n, which, LINE : 2 * LINE, :] = other[:, HEAD:]
        mine = times(rows, 0)
        for j, b in enumerate(blocks):
            at = slice(j * ROWS, (j + 1) * ROWS)
            wide_out[n, which, 2 * LINE + 16 * j : 2 * LINE + 16 * (j + 1), :] = b[FLAT:]
            place(n, line_of(n, q, j), mine[at, :HEAD], mine[at, HEAD:], b[FLAT:])

    def finish(n, which, q):
        for j in range(RING):
            at = j * ROWS
            place(
                n,
                line_of(n, q, j),
                wide_in[n, which, at : at + ROWS, :],
                wide_in[n, which, LINE + at : LINE + at + ROWS, :],
                wide_in[n, which, 2 * LINE + 16 * j : 2 * LINE + 16 * (j + 1), :],
            )

    def scatter(n):
        pltpu.make_async_remote_copy(
            src_ref=own.at[to_of(n)],
            dst_ref=held.at[seq * TP + tp],
            send_sem=send_sem,
            recv_sem=recv_sem.at[seq * TP + tp],
            device_id=(to_of(n), tp),
        ).start()

    def first(n):
        send(n, 0, 0, 0, side_of(n))
        send(n, 0, 0, 1, 0)
        send(n, 0, 0, -1, 0)

    first(0)

    def prepare(n, _):
        put(own, to_of(n), ready(to_of(n)))

        @pl.when(n > 1)
        def _send():
            scatter(n - 1)

        return _

    lax.fori_loop(1, SEQ, prepare, 0)
    scatter(SEQ - 1)

    def when(n, low=0):
        return pl.when((n >= low) & (n < SEQ))

    def step(it, carry):
        n0, n1, n2, n3, n4 = it, it - D1, it - D2, it - D3, it - D4

        @when(n0, 1)
        def _():
            arrive(n0, 0, 0)
            first(n0)

        @pl.when(it == RELAY)
        def _():
            for k in range(1, 5):
                share(k, k, core, partner).wait_recv()
                share(k, k, core, partner).start()

        @when(n1)
        def _():
            way, side = way_of(n1), side_of(n1)
            arrive(n1, 0 - way, 0)
            send(n1, 0 - way, 0, way, 0)
            send(n1, 0 - way, 0, 0, side)
            arrive(n1, way, 0)
            send(n1, way, 0, 0, side)

        @pl.when(it == D2)
        def _():
            for k in range(1, 5):
                share(k, k, 1 - core, partner).wait_recv()

        @when(n2)
        def _():
            side = side_of(n2)
            arrive(n2, 2, 0)
            send(n2, 2, 0, 0, side)
            expand(n2, 0, 0, 0 - side)
            wide_copy(n2, 0, 0 - side).start()

        @when(n3)
        def _():
            side = side_of(n3)
            for p in (0, -1, 1, 2):
                arrive(n3, p, 0 - side)
            expand(n3, 0 - side, 1, side)
            wide_copy(n3, 1, side).start()

        @when(n4)
        def _():
            side = side_of(n4)
            wide_copy(n4, 0, side).wait_recv()
            wide_copy(n4, 1, side).wait_recv()
            finish(n4, 0, side)
            finish(n4, 1, 2)
            for q in range(TP // 4):
                at = pl.multiple_of(seq_of(n4) * UNIT + q * 128, 128)
                part = key_rows[n4, q * 128 : (q + 1) * 128, :].astype(jnp.float32)
                keys_ref[:HEAD, pl.ds(at, 128)] = part.T.astype(jnp.bfloat16)
                rot = rot_rows[n4, q * 64 : (q + 1) * 64, :].astype(jnp.float32).T
                rot = rot.astype(jnp.bfloat16)
                turned = jnp.dot(
                    rot[:ROT], spread[0], preferred_element_type=jnp.float32
                ) + jnp.dot(rot[ROT:], spread[1], preferred_element_type=jnp.float32)
                keys_ref[HEAD:, pl.ds(at, 128)] = turned.astype(jnp.bfloat16)

        return carry

    lax.fori_loop(0, SEQ + D4, step, 0)
    sent = held.at[pl.ds(0, SEQ - 1 + 7 * SEQ)]
    pltpu.make_async_copy(sent, sent, send_sem).wait()
    pltpu.make_async_copy(wide_out, wide_out, wide_send).wait()
    shared = weights.at[pl.ds(0, 4)]
    pltpu.make_async_copy(shared, shared, up_send).wait()


def store(keys_ref, values_ref, keys_out, values_out, sem):
    copies = []
    for i in range(8):
        rows = pl.ds(24 * i, 24)
        copies.append(pltpu.make_async_copy(keys_ref.at[rows], keys_out.at[rows], sem.at[i]))
    for i in range(8):
        rows = pl.ds(1024 * i, 1024)
        copies.append(
            pltpu.make_async_copy(values_ref.at[rows], values_out.at[rows], sem.at[8 + i])
        )
    for copy in copies:
        copy.start()
    for copy in copies:
        copy.wait()


def shards(latents, rotary_rows, latent_gain, key_up, value_up):
    length = SEQ * UNIT
    vmem = pl.BlockSpec(memory_space=pltpu.VMEM)
    keys, values = pl.pallas_call(
        kernel,
        out_shape=(
            pltpu.VMEM((HEAD + ROT, length), jnp.bfloat16),
            pltpu.VMEM((length, HEAD), jnp.bfloat16),
        ),
        in_specs=[pl.BlockSpec(memory_space=pltpu.HBM)] * 5,
        out_specs=(vmem, vmem),
        scratch_shapes=[
            pltpu.VMEM((SEQ, ROWS, WIDTH), jnp.bfloat16),
            pltpu.VMEM((SEQ, ROWS, ROT), jnp.bfloat16),
            pltpu.VMEM((1, WIDTH), jnp.float32),
            pltpu.VMEM((SEQ, PACKED, 128), jnp.bfloat16),
            pltpu.VMEM((SEQ * TP, PACKED, 128), jnp.bfloat16),
            pltpu.VMEM((5, 2, WIDTH, HEAD), jnp.bfloat16),
            pltpu.VMEM((2, 64, 128), jnp.bfloat16),
            pltpu.VMEM((SEQ, UNIT, HEAD), jnp.bfloat16),
            pltpu.VMEM((SEQ, TP * 16, 128), jnp.bfloat16),
            pltpu.VMEM((SEQ, 2, WIDE, 128), jnp.bfloat16),
            pltpu.VMEM((SEQ, 2, WIDE, 128), jnp.bfloat16),
            pltpu.SemaphoreType.DMA((5,)),
            pltpu.SemaphoreType.DMA,
            pltpu.SemaphoreType.DMA((SEQ * TP,)),
            pltpu.SemaphoreType.DMA,
            pltpu.SemaphoreType.DMA((SEQ, 2)),
            pltpu.SemaphoreType.DMA,
            pltpu.SemaphoreType.DMA((5, 2)),
        ],
        compiler_params=pltpu.CompilerParams(
            collective_id=0, has_side_effects=True, vmem_limit_bytes=40 * 2**20
        ),
        name="gather_and_expand",
    )(
        *(
            pltpu.with_memory_space_constraint(a, pltpu.HBM)
            for a in (
                latents,
                rotary_rows,
                latent_gain.reshape(1, WIDTH),
                key_up.reshape(WIDTH, HEAD),
                value_up.reshape(WIDTH, HEAD),
            )
        )
    )
    hbm = pl.BlockSpec(memory_space=pltpu.HBM)
    keys, values = pl.pallas_call(
        store,
        out_shape=(
            jax.ShapeDtypeStruct(keys.shape, keys.dtype),
            jax.ShapeDtypeStruct(values.shape, values.dtype),
        ),
        in_specs=[vmem, vmem],
        out_specs=(hbm, hbm),
        scratch_shapes=[pltpu.SemaphoreType.DMA((16,))],
        compiler_params=pltpu.CompilerParams(vmem_limit_bytes=2**20),
        name="store",
    )(keys, values)
    return keys[None, None], values[None, :, None]


def solution(mesh):
    return jax.shard_map(
        shards,
        mesh=mesh,
        in_specs=(
            P(None, ("seq", "tp"), None),
            P(None, ("seq", "tp"), None),
            P(),
            P(None, "tp", None),
            P(None, "tp", None),
        ),
        out_specs=(P("seq", "tp", None, None), P("seq", None, "tp", None)),
        check_vma=False,
    )
```

```python
import functools

import jax
import jax.numpy as jnp
from jax import lax
from jax.experimental import pallas as pl
from jax.experimental.pallas import tpu as pltpu
from jax.sharding import PartitionSpec as P

SEQ, TP, RING = 16, 16, 4
ROWS, WIDTH, ROT, HEAD = 32, 512, 64, 128
PACKED = ROWS * WIDTH // 128 + ROWS * ROT // 128
CHUNKS = WIDTH // 128
FLAT = CHUNKS * ROWS
LINE = RING * ROWS
WIDE = 2 * LINE + RING * (PACKED - FLAT)
UNIT = TP * ROWS
D1, D2, D3, D4 = 4, 8, 12, 18
RELAY = 3


def kernel(
    lat_hbm, rot_hbm, gain_hbm, wk_hbm, wv_hbm, keys_ref, values_ref,
    lat_ref, rot_ref, gain_ref, own, held, weights, spread,
    key_rows, rot_rows, wide_out, wide_in,
    load_sem, send_sem, first_recv, near_recv, far_recv, line_recv,
    wide_send, wide_recv, up_send, up_recv,
):
    seq, tp = lax.axis_index("seq"), lax.axis_index("tp")
    z, core = seq // 2, seq % 2
    y, x = tp // RING, tp % RING

    def seq_of(n):
        k = n // 2
        dz = ((k + 1) // 2) * (1 - 2 * ((k + 1) % 2))
        return ((z + dz + 8) % 8) * 2 + (core + n) % 2

    to_of = seq_of

    def tp_of(n, p, q):
        first_y = n % 2
        dy = first_y * p + (1 - first_y) * q
        dx = first_y * q + (1 - first_y) * p
        return ((y + dy + RING) % RING) * RING + (x + dx + RING) % RING

    def line_of(n, q, j):
        first_y = n % 2
        at = (first_y * x + (1 - first_y) * y + q + RING) % RING
        return at * (RING - (RING - 1) * first_y) + j * (1 + (RING - 1) * first_y)

    def up_of(n, q):
        return 1 + 2 * (1 - n % 2) + (1 - q) // 2

    def way_of(n):
        return 1 - 2 * ((n // 4) % 2)

    def side_of(n):
        return 1 - 2 * ((n // 2) % 2)

    loads = [
        pltpu.make_async_copy(source, target, load_sem.at[min(i, 3)])
        for i, (source, target) in enumerate(
            (
                (lat_hbm, lat_ref),
                (gain_hbm, gain_ref),
                (rot_hbm, rot_ref),
                (wk_hbm, weights.at[0, 0]),
                (wv_hbm, weights.at[0, 1]),
            )
        )
    ]
    for load in loads:
        load.start()
    barrier = pltpu.get_barrier_semaphore()

    def greet(n, _):
        pl.semaphore_signal(barrier, inc=1, device_id=(seq_of(n), tp))
        return _

    lax.fori_loop(1, SEQ, greet, 0)
    around = [tp_of(0, 1, 0), tp_of(0, -1, 0), tp_of(0, 0, 1), tp_of(0, 0, -1)]
    for target in around:
        pl.semaphore_signal(barrier, inc=1, device_id=(seq, target))

    for load in loads[:3]:
        load.wait()

    def ready(s):
        rows = lat_ref[s].astype(jnp.float32)
        scale = lax.rsqrt(jnp.mean(rows * rows, axis=-1, keepdims=True) + 1e-06)
        rows = (rows * scale * gain_ref[...]).astype(jnp.bfloat16)
        rot = rot_ref[s]
        rot = jnp.concatenate([rot[: ROWS // 2], rot[ROWS // 2 :]], axis=-1)
        return [rows[:, c * 128 : (c + 1) * 128] for c in range(CHUNKS)] + [rot]

    def put(ref, at, parts):
        for c, part in enumerate(parts):
            ref[at, c * ROWS : c * ROWS + part.shape[0], :] = part

    put(held, seq * TP + tp, ready(seq))
    row = lax.broadcasted_iota(jnp.int32, (64, 128), 0)
    lane = lax.broadcasted_iota(jnp.int32, (64, 128), 1)
    for h in range(2):
        at = (row // 16) * 32 + h * 16 + row % 16
        spread[h] = (at == lane).astype(jnp.float32).astype(jnp.bfloat16)
    pltpu.make_async_copy(weights.at[0], weights.at[0], load_sem.at[3]).wait()

    pl.semaphore_wait(barrier, SEQ - 1 + 4)

    def share(source, target, half, device, recv_sem):
        return pltpu.make_async_remote_copy(
            src_ref=weights.at[source, half],
            dst_ref=weights.at[target, half],
            send_sem=up_send,
            recv_sem=recv_sem,
            device_id=device,
        )

    def shared(recv_sem):
        part = weights.at[pl.ds(1, 2)]
        pltpu.make_async_copy(part, part, recv_sem).wait()

    partner = (z * 2 + 1 - core, tp)
    for k, target in enumerate(around):
        back = 1 + k + 1 - 2 * (k % 2)
        share(0, back, core, (seq, target), up_recv.at[0]).start()

    def slot_of(n, p, q):
        return seq_of(n) * TP + tp_of(n, p, q)

    def arrive(recv_sem, blocks):
        part = held.at[pl.ds(0, blocks)]
        pltpu.make_async_copy(part, part, recv_sem).wait()

    def send(n, p, q, dp, dq, recv_sem):
        slot = slot_of(n, p, q)
        pltpu.make_async_remote_copy(
            src_ref=held.at[slot],
            dst_ref=held.at[slot],
            send_sem=send_sem,
            recv_sem=recv_sem.at[n],
            device_id=(seq, tp_of(n, dp, dq)),
        ).start()

    def wide_copy(n, which, q):
        return pltpu.make_async_remote_copy(
            src_ref=wide_out.at[n, which],
            dst_ref=wide_in.at[n, which],
            send_sem=wide_send,
            recv_sem=wide_recv.at[n],
            device_id=(seq, tp_of(n, 0, q)),
        )

    def times(rows, k):
        both = jnp.concatenate([weights[k, 0], weights[k, 1]], axis=-1)
        wide = jnp.dot(rows, both, preferred_element_type=jnp.float32)
        return wide.astype(jnp.bfloat16)

    def place(n, device, keys, values, rot):
        key_rows[n, pl.ds(pl.multiple_of(device * ROWS, ROWS), ROWS), :] = keys
        at = pl.multiple_of(seq_of(n) * UNIT + device * ROWS, ROWS)
        values_ref[pl.ds(at, ROWS), :] = values
        rot_rows[n, pl.ds(pl.multiple_of(device * 16, 16), 16), :] = rot

    def expand(n, q, which, target):
        blocks = [held[seq_of(n) * TP + line_of(n, q, j)] for j in range(RING)]
        rows = jnp.concatenate(
            [
                jnp.concatenate(
                    [b[c * ROWS : (c + 1) * ROWS] for c in range(CHUNKS)], axis=-1
                )
                for b in blocks
            ],
            axis=0,
        )
        other = times(rows, up_of(n, target))
        wide_out[n, which, :LINE, :] = other[:, :HEAD]
        wide_out[n, which, LINE : 2 * LINE, :] = other[:, HEAD:]
        mine = times(rows, 0)
        for j, b in enumerate(blocks):
            at = slice(j * ROWS, (j + 1) * ROWS)
            wide_out[n, which, 2 * LINE + 16 * j : 2 * LINE + 16 * (j + 1), :] = b[FLAT:]
            place(n, line_of(n, q, j), mine[at, :HEAD], mine[at, HEAD:], b[FLAT:])

    def finish(n, which, q):
        for j in range(RING):
            at = j * ROWS
            place(
                n,
                line_of(n, q, j),
                wide_in[n, which, at : at + ROWS, :],
                wide_in[n, which, LINE + at : LINE + at + ROWS, :],
                wide_in[n, which, 2 * LINE + 16 * j : 2 * LINE + 16 * (j + 1), :],
            )

    def scatter(n):
        pltpu.make_async_remote_copy(
            src_ref=own.at[to_of(n)],
            dst_ref=held.at[seq * TP + tp],
            send_sem=send_sem,
            recv_sem=first_recv.at[seq],
            device_id=(to_of(n), tp),
        ).start()

    def first(n):
        send(n, 0, 0, 0, side_of(n), line_recv)
        send(n, 0, 0, 1, 0, near_recv)
        send(n, 0, 0, -1, 0, near_recv)

    first(0)

    def prepare(n, _):
        put(own, to_of(n), ready(to_of(n)))

        @pl.when(n > 1)
        def _send():
            scatter(n - 1)

        return _

    lax.fori_loop(1, SEQ, prepare, 0)
    scatter(SEQ - 1)

    def when(n, low=0):
        return pl.when((n >= low) & (n < SEQ))

    def step(it, carry):
        n0, n1, n2, n3, n4 = it, it - D1, it - D2, it - D3, it - D4

        @when(n0, 1)
        def _():
            arrive(first_recv.at[seq_of(n0)], 1)
            first(n0)

        @pl.when(it == RELAY)
        def _():
            shared(up_recv.at[0])
            for k in range(1, 5):
                share(k, k, core, partner, up_recv.at[1]).start()

        @when(n1)
        def _():
            way, side = way_of(n1), side_of(n1)
            arrive(near_recv.at[n1], 2)
            send(n1, 0 - way, 0, way, 0, far_recv)
            send(n1, 0 - way, 0, 0, side, line_recv)
            send(n1, way, 0, 0, side, line_recv)

        @pl.when(it == D2)
        def _():
            shared(up_recv.at[1])

        @when(n2)
        def _():
            side = side_of(n2)
            arrive(far_recv.at[n2], 1)
            send(n2, 2, 0, 0, side, line_recv)
            expand(n2, 0, 0, 0 - side)
            wide_copy(n2, 0, 0 - side).start()

        @when(n3)
        def _():
            side = side_of(n3)
            arrive(line_recv.at[n3], 4)
            expand(n3, 0 - side, 1, side)
            wide_copy(n3, 1, side).start()

        @when(n4)
        def _():
            side = side_of(n4)
            pltpu.make_async_copy(wide_in.at[n4], wide_in.at[n4], wide_recv.at[n4]).wait()
            finish(n4, 0, side)
            finish(n4, 1, 2)
            for q in range(TP // 4):
                at = pl.multiple_of(seq_of(n4) * UNIT + q * 128, 128)
                part = key_rows[n4, q * 128 : (q + 1) * 128, :].astype(jnp.float32)
                keys_ref[:HEAD, pl.ds(at, 128)] = part.T.astype(jnp.bfloat16)
                rot = rot_rows[n4, q * 64 : (q + 1) * 64, :].astype(jnp.float32).T
                rot = rot.astype(jnp.bfloat16)
                turned = jnp.dot(
                    rot[:ROT], spread[0], preferred_element_type=jnp.float32
                ) + jnp.dot(rot[ROT:], spread[1], preferred_element_type=jnp.float32)
                keys_ref[HEAD:, pl.ds(at, 128)] = turned.astype(jnp.bfloat16)

        return carry

    lax.fori_loop(0, SEQ + D4, step, 0)
    sent = held.at[pl.ds(0, SEQ - 1 + 7 * SEQ)]
    pltpu.make_async_copy(sent, sent, send_sem).wait()
    pltpu.make_async_copy(wide_out, wide_out, wide_send).wait()
    given = weights.at[pl.ds(0, 4)]
    pltpu.make_async_copy(given, given, up_send).wait()


def store(keys_ref, values_ref, keys_out, values_out, sem):
    copies = []
    for i in range(8):
        rows = pl.ds(24 * i, 24)
        copies.append(pltpu.make_async_copy(keys_ref.at[rows], keys_out.at[rows], sem.at[i]))
    for i in range(8):
        rows = pl.ds(1024 * i, 1024)
        copies.append(
            pltpu.make_async_copy(values_ref.at[rows], values_out.at[rows], sem.at[8 + i])
        )
    for copy in copies:
        copy.start()
    for copy in copies:
        copy.wait()


def shards(latents, rotary_rows, latent_gain, key_up, value_up):
    length = SEQ * UNIT
    vmem = pl.BlockSpec(memory_space=pltpu.VMEM)
    keys, values = pl.pallas_call(
        kernel,
        out_shape=(
            pltpu.VMEM((HEAD + ROT, length), jnp.bfloat16),
            pltpu.VMEM((length, HEAD), jnp.bfloat16),
        ),
        in_specs=[pl.BlockSpec(memory_space=pltpu.HBM)] * 5,
        out_specs=(vmem, vmem),
        scratch_shapes=[
            pltpu.VMEM((SEQ, ROWS, WIDTH), jnp.bfloat16),
            pltpu.VMEM((SEQ, ROWS, ROT), jnp.bfloat16),
            pltpu.VMEM((1, WIDTH), jnp.float32),
            pltpu.VMEM((SEQ, PACKED, 128), jnp.bfloat16),
            pltpu.VMEM((SEQ * TP, PACKED, 128), jnp.bfloat16),
            pltpu.VMEM((5, 2, WIDTH, HEAD), jnp.bfloat16),
            pltpu.VMEM((2, 64, 128), jnp.bfloat16),
            pltpu.VMEM((SEQ, UNIT, HEAD), jnp.bfloat16),
            pltpu.VMEM((SEQ, TP * 16, 128), jnp.bfloat16),
            pltpu.VMEM((SEQ, 2, WIDE, 128), jnp.bfloat16),
            pltpu.VMEM((SEQ, 2, WIDE, 128), jnp.bfloat16),
            pltpu.SemaphoreType.DMA((4,)),
            pltpu.SemaphoreType.DMA,
            pltpu.SemaphoreType.DMA((SEQ,)),
            pltpu.SemaphoreType.DMA((SEQ,)),
            pltpu.SemaphoreType.DMA((SEQ,)),
            pltpu.SemaphoreType.DMA((SEQ,)),
            pltpu.SemaphoreType.DMA,
            pltpu.SemaphoreType.DMA((SEQ,)),
            pltpu.SemaphoreType.DMA,
            pltpu.SemaphoreType.DMA((2,)),
        ],
        compiler_params=pltpu.CompilerParams(
            collective_id=0, has_side_effects=True, vmem_limit_bytes=40 * 2**20
        ),
        name="gather_and_expand",
    )(
        *(
            pltpu.with_memory_space_constraint(a, pltpu.HBM)
            for a in (
                latents,
                rotary_rows,
                latent_gain.reshape(1, WIDTH),
                key_up.reshape(WIDTH, HEAD),
                value_up.reshape(WIDTH, HEAD),
            )
        )
    )
    hbm = pl.BlockSpec(memory_space=pltpu.HBM)
    keys, values = pl.pallas_call(
        store,
        out_shape=(
            jax.ShapeDtypeStruct(keys.shape, keys.dtype),
            jax.ShapeDtypeStruct(values.shape, values.dtype),
        ),
        in_specs=[vmem, vmem],
        out_specs=(hbm, hbm),
        scratch_shapes=[pltpu.SemaphoreType.DMA((16,))],
        compiler_params=pltpu.CompilerParams(vmem_limit_bytes=2**20),
        name="store",
    )(keys, values)
    return keys[None, None], values[None, :, None]


def solution(mesh):
    return jax.shard_map(
        shards,
        mesh=mesh,
        in_specs=(
            P(None, ("seq", "tp"), None),
            P(None, ("seq", "tp"), None),
            P(),
            P(None, "tp", None),
            P(None, "tp", None),
        ),
        out_specs=(P("seq", "tp", None, None), P("seq", None, "tp", None)),
        check_vma=False,
    )
```

```python
import functools

import jax
import jax.numpy as jnp
from jax import lax
from jax.experimental import pallas as pl
from jax.experimental.pallas import tpu as pltpu
from jax.sharding import PartitionSpec as P

SEQ, TP, RING = 16, 16, 4
ROWS, WIDTH, ROT, HEAD = 32, 512, 64, 128
PACKED = ROWS * WIDTH // 128 + ROWS * ROT // 128
CHUNKS = WIDTH // 128
FLAT = CHUNKS * ROWS
LINE = RING * ROWS
WIDE = 2 * LINE + RING * (PACKED - FLAT)
UNIT = TP * ROWS
D1, D2, D3, D4 = 4, 8, 12, 18
RELAY = 3
NEAR = 10


def kernel(
    lat_hbm, rot_hbm, gain_hbm, wk_hbm, wv_hbm, keys_ref, values_ref,
    lat_ref, rot_ref, gain_ref, own, held, weights, spread,
    key_rows, rot_rows, wide_out, wide_in,
    past_sem, load_sem, send_sem, first_recv, near_recv, far_recv, line_recv,
    wide_send, wide_recv, up_send, up_recv,
):
    seq, tp = lax.axis_index("seq"), lax.axis_index("tp")
    z, core = seq // 2, seq % 2
    y, x = tp // RING, tp % RING

    def seq_of(n):
        k = n // 2
        dz = ((k + 1) // 2) * (1 - 2 * ((k + 1) % 2))
        return ((z + dz + 8) % 8) * 2 + (core + n) % 2

    to_of = seq_of

    def tp_of(n, p, q):
        first_y = n % 2
        dy = first_y * p + (1 - first_y) * q
        dx = first_y * q + (1 - first_y) * p
        return ((y + dy + RING) % RING) * RING + (x + dx + RING) % RING

    def line_of(n, q, j):
        first_y = n % 2
        at = (first_y * x + (1 - first_y) * y + q + RING) % RING
        return at * (RING - (RING - 1) * first_y) + j * (1 + (RING - 1) * first_y)

    def up_of(n, q):
        return 1 + 2 * (1 - n % 2) + (1 - q) // 2

    def way_of(n):
        return 1 - 2 * ((n // 4) % 2)

    def side_of(n):
        return 1 - 2 * ((n // 2) % 2)

    loads = [
        pltpu.make_async_copy(source, target, load_sem.at[min(i, 3)])
        for i, (source, target) in enumerate(
            (
                (lat_hbm, lat_ref),
                (gain_hbm, gain_ref),
                (rot_hbm, rot_ref),
                (wk_hbm, weights.at[0, 0]),
                (wv_hbm, weights.at[0, 1]),
            )
        )
    ]
    for load in loads:
        load.start()
    barrier = pltpu.get_barrier_semaphore()

    def greet(n, _):
        pl.semaphore_signal(barrier, inc=1, device_id=(seq_of(n), tp))
        return _

    lax.fori_loop(1, NEAR, greet, 0)
    around = [tp_of(0, 1, 0), tp_of(0, -1, 0), tp_of(0, 0, 1), tp_of(0, 0, -1)]
    for target in around:
        pl.semaphore_signal(barrier, inc=1, device_id=(seq, target))

    for load in loads[:3]:
        load.wait()

    def ready(s):
        rows = lat_ref[s].astype(jnp.float32)
        scale = lax.rsqrt(jnp.mean(rows * rows, axis=-1, keepdims=True) + 1e-06)
        rows = (rows * scale * gain_ref[...]).astype(jnp.bfloat16)
        rot = rot_ref[s]
        rot = jnp.concatenate([rot[: ROWS // 2], rot[ROWS // 2 :]], axis=-1)
        return [rows[:, c * 128 : (c + 1) * 128] for c in range(CHUNKS)] + [rot]

    def put(ref, at, parts):
        for c, part in enumerate(parts):
            ref[at, c * ROWS : c * ROWS + part.shape[0], :] = part

    put(held, seq * TP + tp, ready(seq))
    row = lax.broadcasted_iota(jnp.int32, (64, 128), 0)
    lane = lax.broadcasted_iota(jnp.int32, (64, 128), 1)
    for h in range(2):
        at = (row // 16) * 32 + h * 16 + row % 16
        spread[h] = (at == lane).astype(jnp.float32).astype(jnp.bfloat16)
    pltpu.make_async_copy(weights.at[0], weights.at[0], load_sem.at[3]).wait()

    pl.semaphore_wait(barrier, NEAR - 1 + 4)
    for dz in (2, 6):
        pl.semaphore_signal(
            past_sem, inc=1, device_id=(((z + dz) % 8) * 2 + core, tp)
        )

    def share(source, target, half, device, recv_sem):
        return pltpu.make_async_remote_copy(
            src_ref=weights.at[source, half],
            dst_ref=weights.at[target, half],
            send_sem=up_send,
            recv_sem=recv_sem,
            device_id=device,
        )

    def shared(recv_sem):
        part = weights.at[pl.ds(1, 2)]
        pltpu.make_async_copy(part, part, recv_sem).wait()

    partner = (z * 2 + 1 - core, tp)
    for k, target in enumerate(around):
        back = 1 + k + 1 - 2 * (k % 2)
        share(0, back, core, (seq, target), up_recv.at[0]).start()

    def slot_of(n, p, q):
        return seq_of(n) * TP + tp_of(n, p, q)

    def arrive(recv_sem, blocks):
        part = held.at[pl.ds(0, blocks)]
        pltpu.make_async_copy(part, part, recv_sem).wait()

    def send(n, p, q, dp, dq, recv_sem):
        slot = slot_of(n, p, q)
        pltpu.make_async_remote_copy(
            src_ref=held.at[slot],
            dst_ref=held.at[slot],
            send_sem=send_sem,
            recv_sem=recv_sem.at[n],
            device_id=(seq, tp_of(n, dp, dq)),
        ).start()

    def wide_copy(n, which, q):
        return pltpu.make_async_remote_copy(
            src_ref=wide_out.at[n, which],
            dst_ref=wide_in.at[n, which],
            send_sem=wide_send,
            recv_sem=wide_recv.at[n],
            device_id=(seq, tp_of(n, 0, q)),
        )

    def times(rows, k):
        both = jnp.concatenate([weights[k, 0], weights[k, 1]], axis=-1)
        wide = jnp.dot(rows, both, preferred_element_type=jnp.float32)
        return wide.astype(jnp.bfloat16)

    def place(n, device, keys, values, rot):
        key_rows[n, pl.ds(pl.multiple_of(device * ROWS, ROWS), ROWS), :] = keys
        at = pl.multiple_of(seq_of(n) * UNIT + device * ROWS, ROWS)
        values_ref[pl.ds(at, ROWS), :] = values
        rot_rows[n, pl.ds(pl.multiple_of(device * 16, 16), 16), :] = rot

    def expand(n, q, which, target):
        blocks = [held[seq_of(n) * TP + line_of(n, q, j)] for j in range(RING)]
        rows = jnp.concatenate(
            [
                jnp.concatenate(
                    [b[c * ROWS : (c + 1) * ROWS] for c in range(CHUNKS)], axis=-1
                )
                for b in blocks
            ],
            axis=0,
        )
        other = times(rows, up_of(n, target))
        wide_out[n, which, :LINE, :] = other[:, :HEAD]
        wide_out[n, which, LINE : 2 * LINE, :] = other[:, HEAD:]
        mine = times(rows, 0)
        for j, b in enumerate(blocks):
            at = slice(j * ROWS, (j + 1) * ROWS)
            wide_out[n, which, 2 * LINE + 16 * j : 2 * LINE + 16 * (j + 1), :] = b[FLAT:]
            place(n, line_of(n, q, j), mine[at, :HEAD], mine[at, HEAD:], b[FLAT:])

    def finish(n, which, q):
        for j in range(RING):
            at = j * ROWS
            place(
                n,
                line_of(n, q, j),
                wide_in[n, which, at : at + ROWS, :],
                wide_in[n, which, LINE + at : LINE + at + ROWS, :],
                wide_in[n, which, 2 * LINE + 16 * j : 2 * LINE + 16 * (j + 1), :],
            )

    def scatter(n):
        pltpu.make_async_remote_copy(
            src_ref=own.at[to_of(n)],
            dst_ref=held.at[seq * TP + tp],
            send_sem=send_sem,
            recv_sem=first_recv.at[seq],
            device_id=(to_of(n), tp),
        ).start()

    def first(n):
        send(n, 0, 0, 0, side_of(n), line_recv)
        send(n, 0, 0, 1, 0, near_recv)
        send(n, 0, 0, -1, 0, near_recv)

    first(0)

    def prepare(n, _):
        put(own, to_of(n), ready(to_of(n)))

        @pl.when((n > 1) & (n != NEAR))
        def _send():
            scatter(n - 1)

        return _

    lax.fori_loop(1, NEAR, prepare, 0)
    scatter(NEAR - 1)
    pl.semaphore_wait(past_sem, 2)
    lax.fori_loop(NEAR, SEQ, prepare, 0)
    scatter(SEQ - 1)

    def when(n, low=0):
        return pl.when((n >= low) & (n < SEQ))

    def step(it, carry):
        n0, n1, n2, n3, n4 = it, it - D1, it - D2, it - D3, it - D4

        @when(n0, 1)
        def _():
            arrive(first_recv.at[seq_of(n0)], 1)
            first(n0)

        @pl.when(it == RELAY)
        def _():
            shared(up_recv.at[0])
            for k in range(1, 5):
                share(k, k, core, partner, up_recv.at[1]).start()

        @when(n1)
        def _():
            way, side = way_of(n1), side_of(n1)
            arrive(near_recv.at[n1], 2)
            send(n1, 0 - way, 0, way, 0, far_recv)
            send(n1, 0 - way, 0, 0, side, line_recv)
            send(n1, way, 0, 0, side, line_recv)

        @pl.when(it == D2)
        def _():
            shared(up_recv.at[1])

        @when(n2)
        def _():
            side = side_of(n2)
            arrive(far_recv.at[n2], 1)
            send(n2, 2, 0, 0, side, line_recv)
            expand(n2, 0, 0, 0 - side)
            wide_copy(n2, 0, 0 - side).start()

        @when(n3)
        def _():
            side = side_of(n3)
            arrive(line_recv.at[n3], 4)
            expand(n3, 0 - side, 1, side)
            wide_copy(n3, 1, side).start()

        @when(n4)
        def _():
            side = side_of(n4)
            pltpu.make_async_copy(wide_in.at[n4], wide_in.at[n4], wide_recv.at[n4]).wait()
            finish(n4, 0, side)
            finish(n4, 1, 2)
            for q in range(TP // 4):
                at = pl.multiple_of(seq_of(n4) * UNIT + q * 128, 128)
                part = key_rows[n4, q * 128 : (q + 1) * 128, :].astype(jnp.float32)
                keys_ref[:HEAD, pl.ds(at, 128)] = part.T.astype(jnp.bfloat16)
                rot = rot_rows[n4, q * 64 : (q + 1) * 64, :].astype(jnp.float32).T
                rot = rot.astype(jnp.bfloat16)
                turned = jnp.dot(
                    rot[:ROT], spread[0], preferred_element_type=jnp.float32
                ) + jnp.dot(rot[ROT:], spread[1], preferred_element_type=jnp.float32)
                keys_ref[HEAD:, pl.ds(at, 128)] = turned.astype(jnp.bfloat16)

        return carry

    lax.fori_loop(0, SEQ + D4, step, 0)
    sent = held.at[pl.ds(0, SEQ - 1 + 7 * SEQ)]
    pltpu.make_async_copy(sent, sent, send_sem).wait()
    pltpu.make_async_copy(wide_out, wide_out, wide_send).wait()
    given = weights.at[pl.ds(0, 4)]
    pltpu.make_async_copy(given, given, up_send).wait()


def store(keys_ref, values_ref, keys_out, values_out, sem):
    copies = []
    for i in range(8):
        rows = pl.ds(24 * i, 24)
        copies.append(pltpu.make_async_copy(keys_ref.at[rows], keys_out.at[rows], sem.at[i]))
    for i in range(8):
        rows = pl.ds(1024 * i, 1024)
        copies.append(
            pltpu.make_async_copy(values_ref.at[rows], values_out.at[rows], sem.at[8 + i])
        )
    for copy in copies:
        copy.start()
    for copy in copies:
        copy.wait()


def shards(latents, rotary_rows, latent_gain, key_up, value_up):
    length = SEQ * UNIT
    vmem = pl.BlockSpec(memory_space=pltpu.VMEM)
    keys, values = pl.pallas_call(
        kernel,
        out_shape=(
            pltpu.VMEM((HEAD + ROT, length), jnp.bfloat16),
            pltpu.VMEM((length, HEAD), jnp.bfloat16),
        ),
        in_specs=[pl.BlockSpec(memory_space=pltpu.HBM)] * 5,
        out_specs=(vmem, vmem),
        scratch_shapes=[
            pltpu.VMEM((SEQ, ROWS, WIDTH), jnp.bfloat16),
            pltpu.VMEM((SEQ, ROWS, ROT), jnp.bfloat16),
            pltpu.VMEM((1, WIDTH), jnp.float32),
            pltpu.VMEM((SEQ, PACKED, 128), jnp.bfloat16),
            pltpu.VMEM((SEQ * TP, PACKED, 128), jnp.bfloat16),
            pltpu.VMEM((5, 2, WIDTH, HEAD), jnp.bfloat16),
            pltpu.VMEM((2, 64, 128), jnp.bfloat16),
            pltpu.VMEM((SEQ, UNIT, HEAD), jnp.bfloat16),
            pltpu.VMEM((SEQ, TP * 16, 128), jnp.bfloat16),
            pltpu.VMEM((SEQ, 2, WIDE, 128), jnp.bfloat16),
            pltpu.VMEM((SEQ, 2, WIDE, 128), jnp.bfloat16),
            pltpu.SemaphoreType.REGULAR,
            pltpu.SemaphoreType.DMA((4,)),
            pltpu.SemaphoreType.DMA,
            pltpu.SemaphoreType.DMA((SEQ,)),
            pltpu.SemaphoreType.DMA((SEQ,)),
            pltpu.SemaphoreType.DMA((SEQ,)),
            pltpu.SemaphoreType.DMA((SEQ,)),
            pltpu.SemaphoreType.DMA,
            pltpu.SemaphoreType.DMA((SEQ,)),
            pltpu.SemaphoreType.DMA,
            pltpu.SemaphoreType.DMA((2,)),
        ],
        compiler_params=pltpu.CompilerParams(
            collective_id=0, has_side_effects=True, vmem_limit_bytes=40 * 2**20
        ),
        name="gather_and_expand",
    )(
        *(
            pltpu.with_memory_space_constraint(a, pltpu.HBM)
            for a in (
                latents,
                rotary_rows,
                latent_gain.reshape(1, WIDTH),
                key_up.reshape(WIDTH, HEAD),
                value_up.reshape(WIDTH, HEAD),
            )
        )
    )
    hbm = pl.BlockSpec(memory_space=pltpu.HBM)
    keys, values = pl.pallas_call(
        store,
        out_shape=(
            jax.ShapeDtypeStruct(keys.shape, keys.dtype),
            jax.ShapeDtypeStruct(values.shape, values.dtype),
        ),
        in_specs=[vmem, vmem],
        out_specs=(hbm, hbm),
        scratch_shapes=[pltpu.SemaphoreType.DMA((16,))],
        compiler_params=pltpu.CompilerParams(vmem_limit_bytes=2**20),
        name="store",
    )(keys, values)
    return keys[None, None], values[None, :, None]


def solution(mesh):
    return jax.shard_map(
        shards,
        mesh=mesh,
        in_specs=(
            P(None, ("seq", "tp"), None),
            P(None, ("seq", "tp"), None),
            P(),
            P(None, "tp", None),
            P(None, "tp", None),
        ),
        out_specs=(P("seq", "tp", None, None), P("seq", None, "tp", None)),
        check_vma=False,
    )
```

```python
import functools

import jax
import jax.numpy as jnp
from jax import lax
from jax.experimental import pallas as pl
from jax.experimental.pallas import tpu as pltpu
from jax.sharding import PartitionSpec as P

SEQ, TP, RING = 16, 16, 4
ROWS, WIDTH, ROT, HEAD = 32, 512, 64, 128
PACKED = ROWS * WIDTH // 128 + ROWS * ROT // 128
CHUNKS = WIDTH // 128
FLAT = CHUNKS * ROWS
LINE = RING * ROWS
WIDE = 2 * LINE + RING * (PACKED - FLAT)
UNIT = TP * ROWS
D1, D2, D3, D4 = 4, 8, 12, 18
RELAY = 3
AHEAD = 9
NEAR = 10


def kernel(
    lat_hbm, rot_hbm, gain_hbm, wk_hbm, wv_hbm, keys_ref, values_ref,
    lat_ref, rot_ref, gain_ref, own, held, weights, spread,
    key_rows, rot_rows, wide_out, wide_in,
    past_sem, load_sem, send_sem, first_recv, near_recv, far_recv, line_recv,
    wide_send, wide_recv, up_send, up_recv,
):
    seq, tp = lax.axis_index("seq"), lax.axis_index("tp")
    z, core = seq // 2, seq % 2
    y, x = tp // RING, tp % RING

    def seq_of(n):
        k = n // 2
        dz = ((k + 1) // 2) * (1 - 2 * ((k + 1) % 2))
        return ((z + dz + 8) % 8) * 2 + (core + n) % 2

    to_of = seq_of

    def tp_of(n, p, q):
        first_y = n % 2
        dy = first_y * p + (1 - first_y) * q
        dx = first_y * q + (1 - first_y) * p
        return ((y + dy + RING) % RING) * RING + (x + dx + RING) % RING

    def line_of(n, q, j):
        first_y = n % 2
        at = (first_y * x + (1 - first_y) * y + q + RING) % RING
        return at * (RING - (RING - 1) * first_y) + j * (1 + (RING - 1) * first_y)

    def up_of(n, q):
        return 1 + 2 * (1 - n % 2) + (1 - q) // 2

    def way_of(n):
        return 1 - 2 * ((n // 4) % 2)

    def side_of(n):
        return 1 - 2 * ((n // 2) % 2)

    loads = [
        pltpu.make_async_copy(source, target, load_sem.at[min(i, 3)])
        for i, (source, target) in enumerate(
            (
                (lat_hbm, lat_ref),
                (gain_hbm, gain_ref),
                (rot_hbm, rot_ref),
                (wk_hbm, weights.at[0, 0]),
                (wv_hbm, weights.at[0, 1]),
            )
        )
    ]
    for load in loads:
        load.start()
    barrier = pltpu.get_barrier_semaphore()

    def greet(n, _):
        pl.semaphore_signal(barrier, inc=1, device_id=(seq_of(n), tp))
        return _

    lax.fori_loop(1, NEAR, greet, 0)
    around = [tp_of(0, 1, 0), tp_of(0, -1, 0), tp_of(0, 0, 1), tp_of(0, 0, -1)]
    for target in around:
        pl.semaphore_signal(barrier, inc=1, device_id=(seq, target))

    for load in loads[:3]:
        load.wait()

    def ready(s):
        rows = lat_ref[s].astype(jnp.float32)
        scale = lax.rsqrt(jnp.mean(rows * rows, axis=-1, keepdims=True) + 1e-06)
        rows = (rows * scale * gain_ref[...]).astype(jnp.bfloat16)
        rot = rot_ref[s]
        rot = jnp.concatenate([rot[: ROWS // 2], rot[ROWS // 2 :]], axis=-1)
        return [rows[:, c * 128 : (c + 1) * 128] for c in range(CHUNKS)] + [rot]

    def put(ref, at, parts):
        for c, part in enumerate(parts):
            ref[at, c * ROWS : c * ROWS + part.shape[0], :] = part

    put(held, seq * TP + tp, ready(seq))
    row = lax.broadcasted_iota(jnp.int32, (64, 128), 0)
    lane = lax.broadcasted_iota(jnp.int32, (64, 128), 1)
    for h in range(2):
        at = (row // 16) * 32 + h * 16 + row % 16
        spread[h] = (at == lane).astype(jnp.float32).astype(jnp.bfloat16)
    pltpu.make_async_copy(weights.at[0], weights.at[0], load_sem.at[3]).wait()

    def put_own(n, _):
        put(own, to_of(n), ready(to_of(n)))
        return _

    lax.fori_loop(1, AHEAD, put_own, 0)
    pl.semaphore_wait(barrier, NEAR - 1 + 4)
    for dz in (2, 6):
        pl.semaphore_signal(
            past_sem, inc=1, device_id=(((z + dz) % 8) * 2 + core, tp)
        )

    def share(source, target, half, device, recv_sem):
        return pltpu.make_async_remote_copy(
            src_ref=weights.at[source, half],
            dst_ref=weights.at[target, half],
            send_sem=up_send,
            recv_sem=recv_sem,
            device_id=device,
        )

    def shared(recv_sem):
        part = weights.at[pl.ds(1, 2)]
        pltpu.make_async_copy(part, part, recv_sem).wait()

    partner = (z * 2 + 1 - core, tp)
    for k, target in enumerate(around):
        back = 1 + k + 1 - 2 * (k % 2)
        share(0, back, core, (seq, target), up_recv.at[0]).start()

    def slot_of(n, p, q):
        return seq_of(n) * TP + tp_of(n, p, q)

    def arrive(recv_sem, blocks):
        part = held.at[pl.ds(0, blocks)]
        pltpu.make_async_copy(part, part, recv_sem).wait()

    def send(n, p, q, dp, dq, recv_sem):
        slot = slot_of(n, p, q)
        pltpu.make_async_remote_copy(
            src_ref=held.at[slot],
            dst_ref=held.at[slot],
            send_sem=send_sem,
            recv_sem=recv_sem.at[n],
            device_id=(seq, tp_of(n, dp, dq)),
        ).start()

    def wide_copy(n, which, q):
        return pltpu.make_async_remote_copy(
            src_ref=wide_out.at[n, which],
            dst_ref=wide_in.at[n, which],
            send_sem=wide_send,
            recv_sem=wide_recv.at[n],
            device_id=(seq, tp_of(n, 0, q)),
        )

    def times(rows, k):
        both = jnp.concatenate([weights[k, 0], weights[k, 1]], axis=-1)
        wide = jnp.dot(rows, both, preferred_element_type=jnp.float32)
        return wide.astype(jnp.bfloat16)

    def place(n, device, keys, values, rot):
        key_rows[n, pl.ds(pl.multiple_of(device * ROWS, ROWS), ROWS), :] = keys
        at = pl.multiple_of(seq_of(n) * UNIT + device * ROWS, ROWS)
        values_ref[pl.ds(at, ROWS), :] = values
        rot_rows[n, pl.ds(pl.multiple_of(device * 16, 16), 16), :] = rot

    def expand(n, q, which, target):
        blocks = [held[seq_of(n) * TP + line_of(n, q, j)] for j in range(RING)]
        rows = jnp.concatenate(
            [
                jnp.concatenate(
                    [b[c * ROWS : (c + 1) * ROWS] for c in range(CHUNKS)], axis=-1
                )
                for b in blocks
            ],
            axis=0,
        )
        other = times(rows, up_of(n, target))
        wide_out[n, which, :LINE, :] = other[:, :HEAD]
        wide_out[n, which, LINE : 2 * LINE, :] = other[:, HEAD:]
        mine = times(rows, 0)
        for j, b in enumerate(blocks):
            at = slice(j * ROWS, (j + 1) * ROWS)
            wide_out[n, which, 2 * LINE + 16 * j : 2 * LINE + 16 * (j + 1), :] = b[FLAT:]
            place(n, line_of(n, q, j), mine[at, :HEAD], mine[at, HEAD:], b[FLAT:])

    def finish(n, which, q):
        for j in range(RING):
            at = j * ROWS
            place(
                n,
                line_of(n, q, j),
                wide_in[n, which, at : at + ROWS, :],
                wide_in[n, which, LINE + at : LINE + at + ROWS, :],
                wide_in[n, which, 2 * LINE + 16 * j : 2 * LINE + 16 * (j + 1), :],
            )

    def scatter(n):
        pltpu.make_async_remote_copy(
            src_ref=own.at[to_of(n)],
            dst_ref=held.at[seq * TP + tp],
            send_sem=send_sem,
            recv_sem=first_recv.at[seq],
            device_id=(to_of(n), tp),
        ).start()

    def first(n):
        send(n, 0, 0, 0, side_of(n), line_recv)
        send(n, 0, 0, 1, 0, near_recv)
        send(n, 0, 0, -1, 0, near_recv)

    first(0)

    def prepare(n, _):
        put(own, to_of(n), ready(to_of(n)))

        @pl.when((n > 1) & (n != NEAR))
        def _send():
            scatter(n - 1)

        return _

    for n in range(1, AHEAD - 1):
        scatter(n)
    lax.fori_loop(AHEAD, NEAR, prepare, 0)
    scatter(NEAR - 1)
    pl.semaphore_wait(past_sem, 2)
    lax.fori_loop(NEAR, SEQ, prepare, 0)
    scatter(SEQ - 1)

    def when(n, low=0):
        return pl.when((n >= low) & (n < SEQ))

    def step(it, carry):
        n0, n1, n2, n3, n4 = it, it - D1, it - D2, it - D3, it - D4

        @when(n0, 1)
        def _():
            arrive(first_recv.at[seq_of(n0)], 1)
            first(n0)

        @pl.when(it == RELAY)
        def _():
            shared(up_recv.at[0])
            for k in range(1, 5):
                share(k, k, core, partner, up_recv.at[1]).start()

        @when(n1)
        def _():
            way, side = way_of(n1), side_of(n1)
            arrive(near_recv.at[n1], 2)
            send(n1, 0 - way, 0, way, 0, far_recv)
            send(n1, 0 - way, 0, 0, side, line_recv)
            send(n1, way, 0, 0, side, line_recv)

        @pl.when(it == D2)
        def _():
            shared(up_recv.at[1])

        @when(n2)
        def _():
            side = side_of(n2)
            arrive(far_recv.at[n2], 1)
            send(n2, 2, 0, 0, side, line_recv)
            expand(n2, 0, 0, 0 - side)
            wide_copy(n2, 0, 0 - side).start()

        @when(n3)
        def _():
            side = side_of(n3)
            arrive(line_recv.at[n3], 4)
            expand(n3, 0 - side, 1, side)
            wide_copy(n3, 1, side).start()

        @when(n4)
        def _():
            side = side_of(n4)
            pltpu.make_async_copy(wide_in.at[n4], wide_in.at[n4], wide_recv.at[n4]).wait()
            finish(n4, 0, side)
            finish(n4, 1, 2)
            for q in range(TP // 4):
                at = pl.multiple_of(seq_of(n4) * UNIT + q * 128, 128)
                part = key_rows[n4, q * 128 : (q + 1) * 128, :].astype(jnp.float32)
                keys_ref[:HEAD, pl.ds(at, 128)] = part.T.astype(jnp.bfloat16)
                rot = rot_rows[n4, q * 64 : (q + 1) * 64, :].astype(jnp.float32).T
                rot = rot.astype(jnp.bfloat16)
                turned = jnp.dot(
                    rot[:ROT], spread[0], preferred_element_type=jnp.float32
                ) + jnp.dot(rot[ROT:], spread[1], preferred_element_type=jnp.float32)
                keys_ref[HEAD:, pl.ds(at, 128)] = turned.astype(jnp.bfloat16)

        return carry

    lax.fori_loop(0, SEQ + D4, step, 0)
    sent = held.at[pl.ds(0, SEQ - 1 + 7 * SEQ)]
    pltpu.make_async_copy(sent, sent, send_sem).wait()
    pltpu.make_async_copy(wide_out, wide_out, wide_send).wait()
    given = weights.at[pl.ds(0, 4)]
    pltpu.make_async_copy(given, given, up_send).wait()


def store(keys_ref, values_ref, keys_out, values_out, sem):
    copies = []
    for i in range(8):
        rows = pl.ds(24 * i, 24)
        copies.append(pltpu.make_async_copy(keys_ref.at[rows], keys_out.at[rows], sem.at[i]))
    for i in range(8):
        rows = pl.ds(1024 * i, 1024)
        copies.append(
            pltpu.make_async_copy(values_ref.at[rows], values_out.at[rows], sem.at[8 + i])
        )
    for copy in copies:
        copy.start()
    for copy in copies:
        copy.wait()


def shards(latents, rotary_rows, latent_gain, key_up, value_up):
    length = SEQ * UNIT
    vmem = pl.BlockSpec(memory_space=pltpu.VMEM)
    keys, values = pl.pallas_call(
        kernel,
        out_shape=(
            pltpu.VMEM((HEAD + ROT, length), jnp.bfloat16),
            pltpu.VMEM((length, HEAD), jnp.bfloat16),
        ),
        in_specs=[pl.BlockSpec(memory_space=pltpu.HBM)] * 5,
        out_specs=(vmem, vmem),
        scratch_shapes=[
            pltpu.VMEM((SEQ, ROWS, WIDTH), jnp.bfloat16),
            pltpu.VMEM((SEQ, ROWS, ROT), jnp.bfloat16),
            pltpu.VMEM((1, WIDTH), jnp.float32),
            pltpu.VMEM((SEQ, PACKED, 128), jnp.bfloat16),
            pltpu.VMEM((SEQ * TP, PACKED, 128), jnp.bfloat16),
            pltpu.VMEM((5, 2, WIDTH, HEAD), jnp.bfloat16),
            pltpu.VMEM((2, 64, 128), jnp.bfloat16),
            pltpu.VMEM((SEQ, UNIT, HEAD), jnp.bfloat16),
            pltpu.VMEM((SEQ, TP * 16, 128), jnp.bfloat16),
            pltpu.VMEM((SEQ, 2, WIDE, 128), jnp.bfloat16),
            pltpu.VMEM((SEQ, 2, WIDE, 128), jnp.bfloat16),
            pltpu.SemaphoreType.REGULAR,
            pltpu.SemaphoreType.DMA((4,)),
            pltpu.SemaphoreType.DMA,
            pltpu.SemaphoreType.DMA((SEQ,)),
            pltpu.SemaphoreType.DMA((SEQ,)),
            pltpu.SemaphoreType.DMA((SEQ,)),
            pltpu.SemaphoreType.DMA((SEQ,)),
            pltpu.SemaphoreType.DMA,
            pltpu.SemaphoreType.DMA((SEQ,)),
            pltpu.SemaphoreType.DMA,
            pltpu.SemaphoreType.DMA((2,)),
        ],
        compiler_params=pltpu.CompilerParams(
            collective_id=0, has_side_effects=True, vmem_limit_bytes=40 * 2**20
        ),
        name="gather_and_expand",
    )(
        *(
            pltpu.with_memory_space_constraint(a, pltpu.HBM)
            for a in (
                latents,
                rotary_rows,
                latent_gain.reshape(1, WIDTH),
                key_up.reshape(WIDTH, HEAD),
                value_up.reshape(WIDTH, HEAD),
            )
        )
    )
    hbm = pl.BlockSpec(memory_space=pltpu.HBM)
    keys, values = pl.pallas_call(
        store,
        out_shape=(
            jax.ShapeDtypeStruct(keys.shape, keys.dtype),
            jax.ShapeDtypeStruct(values.shape, values.dtype),
        ),
        in_specs=[vmem, vmem],
        out_specs=(hbm, hbm),
        scratch_shapes=[pltpu.SemaphoreType.DMA((16,))],
        compiler_params=pltpu.CompilerParams(vmem_limit_bytes=2**20),
        name="store",
    )(keys, values)
    return keys[None, None], values[None, :, None]


def solution(mesh):
    return jax.shard_map(
        shards,
        mesh=mesh,
        in_specs=(
            P(None, ("seq", "tp"), None),
            P(None, ("seq", "tp"), None),
            P(),
            P(None, "tp", None),
            P(None, "tp", None),
        ),
        out_specs=(P("seq", "tp", None, None), P("seq", None, "tp", None)),
        check_vma=False,
    )
```

```python
import functools

import jax
import jax.numpy as jnp
from jax import lax
from jax.experimental import pallas as pl
from jax.experimental.pallas import tpu as pltpu
from jax.sharding import PartitionSpec as P

SEQ, TP, RING = 16, 16, 4
ROWS, WIDTH, ROT, HEAD = 32, 512, 64, 128
PACKED = ROWS * WIDTH // 128 + ROWS * ROT // 128
CHUNKS = WIDTH // 128
FLAT = CHUNKS * ROWS
LINE = RING * ROWS
WIDE = 2 * LINE + RING * (PACKED - FLAT)
UNIT = TP * ROWS
D1, D2, D3, D4 = 4, 8, 12, 17
RELAY = 5
NEAR = 10


def kernel(
    lat_hbm, rot_hbm, gain_hbm, wk_hbm, wv_hbm, keys_ref, values_ref,
    lat_ref, rot_ref, gain_ref, own, held, weights, spread,
    key_rows, rot_rows, wide_out, wide_in,
    past_sem, load_sem, send_sem, first_recv, near_recv, far_recv, line_recv,
    wide_send, wide_recv, up_send, up_recv,
):
    seq, tp = lax.axis_index("seq"), lax.axis_index("tp")
    z, core = seq // 2, seq % 2
    y, x = tp // RING, tp % RING

    def seq_of(n):
        k = n // 2
        dz = ((k + 1) // 2) * (1 - 2 * ((k + 1) % 2))
        return ((z + dz + 8) % 8) * 2 + (core + n) % 2

    to_of = seq_of

    def tp_of(n, p, q):
        first_y = n % 2
        dy = first_y * p + (1 - first_y) * q
        dx = first_y * q + (1 - first_y) * p
        return ((y + dy + RING) % RING) * RING + (x + dx + RING) % RING

    def line_of(n, q, j):
        first_y = n % 2
        at = (first_y * x + (1 - first_y) * y + q + RING) % RING
        return at * (RING - (RING - 1) * first_y) + j * (1 + (RING - 1) * first_y)

    def up_of(n, q):
        return 1 + 2 * (1 - n % 2) + (1 - q) // 2

    def way_of(n):
        return 1 - 2 * ((n // 4) % 2)

    def side_of(n):
        return 1 - 2 * ((n // 2) % 2)

    loads = [
        pltpu.make_async_copy(source, target, load_sem.at[min(i, 3)])
        for i, (source, target) in enumerate(
            (
                (lat_hbm, lat_ref),
                (gain_hbm, gain_ref),
                (rot_hbm, rot_ref),
                (wk_hbm, weights.at[0, 0]),
                (wv_hbm, weights.at[0, 1]),
            )
        )
    ]
    for load in loads:
        load.start()
    barrier = pltpu.get_barrier_semaphore()

    def greet(n, _):
        pl.semaphore_signal(barrier, inc=1, device_id=(seq_of(n), tp))
        return _

    lax.fori_loop(1, NEAR, greet, 0)
    around = [tp_of(0, 1, 0), tp_of(0, -1, 0), tp_of(0, 0, 1), tp_of(0, 0, -1)]
    for target in around:
        pl.semaphore_signal(barrier, inc=1, device_id=(seq, target))

    for load in loads[:3]:
        load.wait()

    def ready(s):
        rows = lat_ref[s].astype(jnp.float32)
        scale = lax.rsqrt(jnp.mean(rows * rows, axis=-1, keepdims=True) + 1e-06)
        rows = (rows * scale * gain_ref[...]).astype(jnp.bfloat16)
        rot = rot_ref[s]
        rot = jnp.concatenate([rot[: ROWS // 2], rot[ROWS // 2 :]], axis=-1)
        return [rows[:, c * 128 : (c + 1) * 128] for c in range(CHUNKS)] + [rot]

    def put(ref, at, parts):
        for c, part in enumerate(parts):
            ref[at, c * ROWS : c * ROWS + part.shape[0], :] = part

    put(held, seq * TP + tp, ready(seq))
    row = lax.broadcasted_iota(jnp.int32, (64, 128), 0)
    lane = lax.broadcasted_iota(jnp.int32, (64, 128), 1)
    for h in range(2):
        at = (row // 16) * 32 + h * 16 + row % 16
        spread[h] = (at == lane).astype(jnp.float32).astype(jnp.bfloat16)
    pltpu.make_async_copy(weights.at[0], weights.at[0], load_sem.at[3]).wait()

    pl.semaphore_wait(barrier, NEAR - 1 + 4)
    for dz in (2, 6):
        pl.semaphore_signal(
            past_sem, inc=1, device_id=(((z + dz) % 8) * 2 + core, tp)
        )

    def share(source, target, half, device, recv_sem):
        return pltpu.make_async_remote_copy(
            src_ref=weights.at[source, half],
            dst_ref=weights.at[target, half],
            send_sem=up_send,
            recv_sem=recv_sem,
            device_id=device,
        )

    def shared(recv_sem):
        part = weights.at[pl.ds(1, 2)]
        pltpu.make_async_copy(part, part, recv_sem).wait()

    partner = (z * 2 + 1 - core, tp)
    for k, target in enumerate(around):
        back = 1 + k + 1 - 2 * (k % 2)
        share(0, back, core, (seq, target), up_recv.at[0]).start()

    def slot_of(n, p, q):
        return seq_of(n) * TP + tp_of(n, p, q)

    def arrive(recv_sem, blocks):
        part = held.at[pl.ds(0, blocks)]
        pltpu.make_async_copy(part, part, recv_sem).wait()

    def send(n, p, q, dp, dq, recv_sem):
        slot = slot_of(n, p, q)
        pltpu.make_async_remote_copy(
            src_ref=held.at[slot],
            dst_ref=held.at[slot],
            send_sem=send_sem,
            recv_sem=recv_sem.at[n],
            device_id=(seq, tp_of(n, dp, dq)),
        ).start()

    def wide_copy(n, which, q):
        return pltpu.make_async_remote_copy(
            src_ref=wide_out.at[n, which],
            dst_ref=wide_in.at[n, which],
            send_sem=wide_send,
            recv_sem=wide_recv.at[n],
            device_id=(seq, tp_of(n, 0, q)),
        )

    def times(rows, k):
        both = jnp.concatenate([weights[k, 0], weights[k, 1]], axis=-1)
        wide = jnp.dot(rows, both, preferred_element_type=jnp.float32)
        return wide.astype(jnp.bfloat16)

    def place(n, device, keys, values, rot):
        key_rows[n, pl.ds(pl.multiple_of(device * ROWS, ROWS), ROWS), :] = keys
        at = pl.multiple_of(seq_of(n) * UNIT + device * ROWS, ROWS)
        values_ref[pl.ds(at, ROWS), :] = values
        rot_rows[n, pl.ds(pl.multiple_of(device * 16, 16), 16), :] = rot

    def expand(n, q, which, target):
        blocks = [held[seq_of(n) * TP + line_of(n, q, j)] for j in range(RING)]
        rows = jnp.concatenate(
            [
                jnp.concatenate(
                    [b[c * ROWS : (c + 1) * ROWS] for c in range(CHUNKS)], axis=-1
                )
                for b in blocks
            ],
            axis=0,
        )
        other = times(rows, up_of(n, target))
        wide_out[n, which, :LINE, :] = other[:, :HEAD]
        wide_out[n, which, LINE : 2 * LINE, :] = other[:, HEAD:]
        mine = times(rows, 0)
        for j, b in enumerate(blocks):
            at = slice(j * ROWS, (j + 1) * ROWS)
            wide_out[n, which, 2 * LINE + 16 * j : 2 * LINE + 16 * (j + 1), :] = b[FLAT:]
            place(n, line_of(n, q, j), mine[at, :HEAD], mine[at, HEAD:], b[FLAT:])

    def finish(n, which, q):
        for j in range(RING):
            at = j * ROWS
            place(
                n,
                line_of(n, q, j),
                wide_in[n, which, at : at + ROWS, :],
                wide_in[n, which, LINE + at : LINE + at + ROWS, :],
                wide_in[n, which, 2 * LINE + 16 * j : 2 * LINE + 16 * (j + 1), :],
            )

    def scatter(n):
        pltpu.make_async_remote_copy(
            src_ref=own.at[to_of(n)],
            dst_ref=held.at[seq * TP + tp],
            send_sem=send_sem,
            recv_sem=first_recv.at[z],
            device_id=(to_of(n), tp),
        ).start()

    def first(n):
        send(n, 0, 0, 0, side_of(n), line_recv)
        send(n, 0, 0, 1, 0, near_recv)
        send(n, 0, 0, -1, 0, near_recv)

    first(0)

    def prepare(n, _):
        put(own, to_of(n), ready(to_of(n)))

        @pl.when((n > 1) & (n != NEAR))
        def _send():
            scatter(n - 1)

        return _

    lax.fori_loop(1, NEAR, prepare, 0)
    scatter(NEAR - 1)
    pl.semaphore_wait(past_sem, 2)
    lax.fori_loop(NEAR, SEQ, prepare, 0)
    scatter(SEQ - 1)

    def when(n, low=0):
        return pl.when((n >= low) & (n < SEQ))

    def step(it, carry):
        n0, n1, n2, n3, n4 = it, it - D1, it - D2, it - D3, it - D4

        @pl.when(n0 == 1)
        def _():
            arrive(first_recv.at[z], 1)

        @pl.when((n0 > 1) & (n0 < SEQ) & (n0 % 2 == 0))
        def _():
            arrive(first_recv.at[seq_of(n0) // 2], 2)

        @when(n0, 1)
        def _():
            first(n0)

        @pl.when(it == RELAY)
        def _():
            shared(up_recv.at[0])
            for k in range(1, 5):
                share(k, k, core, partner, up_recv.at[1]).start()

        @when(n1)
        def _():
            way, side = way_of(n1), side_of(n1)
            arrive(near_recv.at[n1], 2)
            send(n1, 0 - way, 0, way, 0, far_recv)
            send(n1, 0 - way, 0, 0, side, line_recv)
            send(n1, way, 0, 0, side, line_recv)

        @pl.when(it == D2)
        def _():
            shared(up_recv.at[1])

        @when(n2)
        def _():
            side = side_of(n2)
            arrive(far_recv.at[n2], 1)
            send(n2, 2, 0, 0, side, line_recv)
            expand(n2, 0, 0, 0 - side)
            wide_copy(n2, 0, 0 - side).start()

        @when(n3)
        def _():
            side = side_of(n3)
            arrive(line_recv.at[n3], 4)
            expand(n3, 0 - side, 1, side)
            wide_copy(n3, 1, side).start()

        @when(n4)
        def _():
            side = side_of(n4)
            pltpu.make_async_copy(wide_in.at[n4], wide_in.at[n4], wide_recv.at[n4]).wait()
            finish(n4, 0, side)
            finish(n4, 1, 2)
            for q in range(TP // 4):
                at = pl.multiple_of(seq_of(n4) * UNIT + q * 128, 128)
                part = key_rows[n4, q * 128 : (q + 1) * 128, :].astype(jnp.float32)
                keys_ref[:HEAD, pl.ds(at, 128)] = part.T.astype(jnp.bfloat16)
                rot = rot_rows[n4, q * 64 : (q + 1) * 64, :].astype(jnp.float32).T
                rot = rot.astype(jnp.bfloat16)
                turned = jnp.dot(
                    rot[:ROT], spread[0], preferred_element_type=jnp.float32
                ) + jnp.dot(rot[ROT:], spread[1], preferred_element_type=jnp.float32)
                keys_ref[HEAD:, pl.ds(at, 128)] = turned.astype(jnp.bfloat16)

        return carry

    lax.fori_loop(0, SEQ + D4, step, 0)
    sent = held.at[pl.ds(0, SEQ - 1 + 7 * SEQ)]
    pltpu.make_async_copy(sent, sent, send_sem).wait()
    pltpu.make_async_copy(wide_out, wide_out, wide_send).wait()
    given = weights.at[pl.ds(0, 4)]
    pltpu.make_async_copy(given, given, up_send).wait()


def store(keys_ref, values_ref, keys_out, values_out, sem):
    copies = []
    for i in range(8):
        rows = pl.ds(24 * i, 24)
        copies.append(pltpu.make_async_copy(keys_ref.at[rows], keys_out.at[rows], sem.at[i]))
    for i in range(8):
        rows = pl.ds(1024 * i, 1024)
        copies.append(
            pltpu.make_async_copy(values_ref.at[rows], values_out.at[rows], sem.at[8 + i])
        )
    for copy in copies:
        copy.start()
    for copy in copies:
        copy.wait()


def shards(latents, rotary_rows, latent_gain, key_up, value_up):
    length = SEQ * UNIT
    vmem = pl.BlockSpec(memory_space=pltpu.VMEM)
    keys, values = pl.pallas_call(
        kernel,
        out_shape=(
            pltpu.VMEM((HEAD + ROT, length), jnp.bfloat16),
            pltpu.VMEM((length, HEAD), jnp.bfloat16),
        ),
        in_specs=[pl.BlockSpec(memory_space=pltpu.HBM)] * 5,
        out_specs=(vmem, vmem),
        scratch_shapes=[
            pltpu.VMEM((SEQ, ROWS, WIDTH), jnp.bfloat16),
            pltpu.VMEM((SEQ, ROWS, ROT), jnp.bfloat16),
            pltpu.VMEM((1, WIDTH), jnp.float32),
            pltpu.VMEM((SEQ, PACKED, 128), jnp.bfloat16),
            pltpu.VMEM((SEQ * TP, PACKED, 128), jnp.bfloat16),
            pltpu.VMEM((5, 2, WIDTH, HEAD), jnp.bfloat16),
            pltpu.VMEM((2, 64, 128), jnp.bfloat16),
            pltpu.VMEM((SEQ, UNIT, HEAD), jnp.bfloat16),
            pltpu.VMEM((SEQ, TP * 16, 128), jnp.bfloat16),
            pltpu.VMEM((SEQ, 2, WIDE, 128), jnp.bfloat16),
            pltpu.VMEM((SEQ, 2, WIDE, 128), jnp.bfloat16),
            pltpu.SemaphoreType.REGULAR,
            pltpu.SemaphoreType.DMA((4,)),
            pltpu.SemaphoreType.DMA,
            pltpu.SemaphoreType.DMA((SEQ // 2,)),
            pltpu.SemaphoreType.DMA((SEQ,)),
            pltpu.SemaphoreType.DMA((SEQ,)),
            pltpu.SemaphoreType.DMA((SEQ,)),
            pltpu.SemaphoreType.DMA,
            pltpu.SemaphoreType.DMA((SEQ,)),
            pltpu.SemaphoreType.DMA,
            pltpu.SemaphoreType.DMA((2,)),
        ],
        compiler_params=pltpu.CompilerParams(
            collective_id=0, has_side_effects=True, vmem_limit_bytes=40 * 2**20
        ),
        name="gather_and_expand",
    )(
        *(
            pltpu.with_memory_space_constraint(a, pltpu.HBM)
            for a in (
                latents,
                rotary_rows,
                latent_gain.reshape(1, WIDTH),
                key_up.reshape(WIDTH, HEAD),
                value_up.reshape(WIDTH, HEAD),
            )
        )
    )
    hbm = pl.BlockSpec(memory_space=pltpu.HBM)
    keys, values = pl.pallas_call(
        store,
        out_shape=(
            jax.ShapeDtypeStruct(keys.shape, keys.dtype),
            jax.ShapeDtypeStruct(values.shape, values.dtype),
        ),
        in_specs=[vmem, vmem],
        out_specs=(hbm, hbm),
        scratch_shapes=[pltpu.SemaphoreType.DMA((16,))],
        compiler_params=pltpu.CompilerParams(vmem_limit_bytes=2**20),
        name="store",
    )(keys, values)
    return keys[None, None], values[None, :, None]


def solution(mesh):
    return jax.shard_map(
        shards,
        mesh=mesh,
        in_specs=(
            P(None, ("seq", "tp"), None),
            P(None, ("seq", "tp"), None),
            P(),
            P(None, "tp", None),
            P(None, "tp", None),
        ),
        out_specs=(P("seq", "tp", None, None), P("seq", None, "tp", None)),
        check_vma=False,
    )
```
